256 devices in a mesh: rep: 64 (over z, x, core), batch: 4 (over y).
Axes of the slice: x: 4, y: 4, z: 8, core: 2. Of those that a mesh axis runs over, the one named last changes fastest.
Arguments:
- embed: bfloat16 [32768, 1024], P(('rep', 'batch')), may hold values from -9 to 9
- actions: int32 [32768, 5], P(('rep', 'batch')), may hold values from 0 to 17
- rewards: float32 [32768, 5], P(('rep', 'batch')), may hold values from -1 to 1
- ends: int32 [32768, 5], P(('rep', 'batch')), may hold values 0 or 1
- behaviour: float32 [32768, 5, 18], P(('rep', 'batch')), may hold values from -5 to 5
- w_hidden: bfloat16 [1024, 1024], replicated, may hold values from -0.1875 to 0.1875
- w_action: bfloat16 [18, 1024], replicated, may hold values from -3 to 3
- w_heads: bfloat16 [1024, 36], replicated, may hold values from -0.1875 to 0.1875
Outputs:
- grad_hidden: float32 [1024, 1024], replicated
- grad_action: float32 [18, 1024], replicated
- grad_heads: float32 [1024, 36], replicated
- targets: float32 [32768, 5], P(('rep', 'batch'))
The draws below stay inside these ranges and needn't reach their ends.
All inputs are finite; a program needn't handle non-finite values. No bound on the sum of `ends` on one device may be relied on, other than what follows from the above.
Results may differ from the reference program's by a relative error of at most 0.0057.
Values sent between devices are 32-bit elements; how exact they have to be, the bound alone decides.
No kernel may reach another device: no remote copies, remote signals or barrier semaphores. Data moves between devices by JAX's collectives and lax.ppermute only.
A program may use at most 64 MiB of HBM per device.

```python
import jax
import jax.numpy as jnp
from jax import lax

HID = 1024
ACTIONS = 18
STEPS = 5
B_DEV = 128
TOTAL = 32768
N_REP = 64
N_BATCH = 4
DEVICES = 256


def draw_embed(key, part):
    key_here = jax.random.fold_in(key, 7)
    row_ids = jnp.arange(TOTAL, dtype=jnp.int32)
    lane = row_ids // B_DEV % N_BATCH
    frac = lane.astype(jnp.float32) / float(max(N_BATCH - 1, 1))
    base = jnp.clip(jax.random.normal(key_here, (TOTAL, HID), jnp.float32), -6.0, 6.0)
    scale = 0.5 * jnp.power(3.0, frac)
    return (base * scale[:, None]).astype(jnp.bfloat16)


def place_ends(result, key, low, high):
    longest = result.shape.index(max(result.shape))
    spots = []
    for shift in (0, 1):
        where = [jax.random.randint(jax.random.fold_in(key, axis), (), 0, length) for axis, length in enumerate(result.shape)]
        where[longest] = (where[longest] + shift) % result.shape[longest]
        spots.append(tuple(where))
    return result.at[spots[0]].set(low).at[spots[1]].set(high)


def block_scale(own_key, extent, shards, smallest, high):
    loudness = 1.0
    for dim, parts in shards:
        steps = jax.random.uniform(jax.random.fold_in(jax.random.fold_in(own_key, 6), dim), (parts,), jnp.float32, smallest / len(shards), high / len(shards))
        loudness = loudness * jnp.repeat(jnp.exp(steps), extent[dim] // parts).reshape((-1,) + (1,) * (len(extent) - 1 - dim))
    return loudness


def noise(rng, dims, scale, reach, pieces=(), kind=jnp.bfloat16):
    result = jax.random.normal(rng, dims, jnp.float32) * scale
    if len(pieces) > 0:
        result = block_scale(rng, dims, pieces, -0.22, 0.18) * result
    return jnp.clip(result, min=-reach, max=reach).astype(kind)


def setup_inputs(seed: int = 0) -> dict:
    streams_of = jax.random.split(jax.random.key(seed), 9)
    return {
        "embed": draw_embed(jax.random.fold_in(streams_of[8], 71), 0),
        "actions": place_ends(jax.random.randint(streams_of[1], (TOTAL, STEPS), 0, ACTIONS), jax.random.fold_in(streams_of[1], 1), 0, ACTIONS - 1).astype(jnp.int32),
        "rewards": jnp.clip(jax.random.uniform(streams_of[2], (TOTAL, STEPS), jnp.float32, -1.0, 1.0) * block_scale(streams_of[2], (TOTAL, STEPS), ((0, 256),), -0.4, 0.0), -1.0, 1.0),
        "ends": place_ends((jax.random.randint(streams_of[3], (TOTAL, STEPS), 0, 8) < 1).astype(jnp.int32), jax.random.fold_in(streams_of[3], 1), 0, 1),
        "behaviour": noise(streams_of[4], (TOTAL, STEPS, ACTIONS), 1.0, 5.0, ((0, 256),), jnp.float32),
        "w_hidden": noise(streams_of[5], (HID, HID), HID ** -0.5, 0.1875),
        "w_action": noise(streams_of[6], (ACTIONS, HID), 0.5, 3.0),
        "w_heads": noise(streams_of[7], (HID, 2 * ACTIONS), HID ** -0.5, 0.1875),
    }


DISCOUNT = 0.997
TRACE_LAMBDA = 0.95
EPSILON = 1e-06

def unroll(emb_block, act_block, w_hidden, w_action, w_heads):
    act_count = w_action.shape[0]
    unroll_len = act_block.shape[1]
    onehot = (act_block[:, :, None] == jnp.arange(act_count, dtype=jnp.int32)[None, None, :]).astype(jnp.bfloat16)
    hidden_state = emb_block.astype(jnp.float32)
    rounded = []
    squashed = []
    head_out = []
    for step in range(unroll_len):
        state_bf16 = hidden_state.astype(jnp.bfloat16)
        rounded.append(state_bf16)
        head_out.append(jnp.dot(state_bf16, w_heads, preferred_element_type=jnp.float32))
        preact = jnp.dot(state_bf16, w_hidden, preferred_element_type=jnp.float32)
        preact = preact + jnp.dot(onehot[:, step], w_action, preferred_element_type=jnp.float32)
        squash = jnp.tanh(preact)
        squashed.append(squash)
        hidden_state = hidden_state + squash
    state_bf16 = hidden_state.astype(jnp.bfloat16)
    head_out.append(jnp.dot(state_bf16, w_heads, preferred_element_type=jnp.float32))
    return (jnp.stack(head_out), rounded, squashed, onehot)

def estimates(head_out, actions, rewards, ends, behaviour):
    act_count = behaviour.shape[-1]
    unroll_len = actions.shape[1]
    logits = head_out[:, :, :act_count]
    qvalues = head_out[:, :, act_count:]
    exp_logits = jnp.exp(logits)
    policy = exp_logits / lax.optimization_barrier(jnp.sum(exp_logits, axis=-1, keepdims=True))
    values = lax.optimization_barrier(jnp.sum(policy * qvalues, axis=-1))
    onehot_f = (jnp.transpose(actions)[:, :, None] == jnp.arange(act_count, dtype=jnp.int32)[None, None, :]).astype(jnp.float32)
    logpol = logits[:unroll_len] - jnp.log(lax.optimization_barrier(jnp.sum(exp_logits[:unroll_len], axis=-1, keepdims=True)))
    behave = jnp.transpose(behaviour, (1, 0, 2))
    behave_log = behave - jnp.log(lax.optimization_barrier(jnp.sum(jnp.exp(behave), axis=-1, keepdims=True)))
    ratios = jnp.exp(lax.optimization_barrier(jnp.sum(onehot_f * (logpol - behave_log), axis=-1)))
    clipped = jnp.minimum(1.0, ratios)
    not_ended = 1.0 - jnp.transpose(ends).astype(jnp.float32)
    td_error = jnp.transpose(rewards) + DISCOUNT * not_ended * values[1:] - values[:unroll_len]
    carried = jnp.zeros_like(values[0])
    collected = []
    for step in range(unroll_len - 1, -1, -1):
        carried = clipped[step] * td_error[step] + DISCOUNT * TRACE_LAMBDA * not_ended[step] * clipped[step] * carried
        collected.append(carried)
    collected = jnp.stack(collected[::-1])
    targets = values[:unroll_len] + collected
    advantage = qvalues[:unroll_len] - values[:unroll_len, :, None]
    return (policy[:unroll_len], onehot_f, targets, advantage)

def objective(head_out, onehot_f, targets, cmpo_policy, taken_weight, norm_scale):
    act_count = onehot_f.shape[-1]
    unroll_len = onehot_f.shape[0]
    logits = head_out[:unroll_len, :, :act_count]
    qvalues = head_out[:unroll_len, :, act_count:]
    logpol = logits - jnp.log(lax.optimization_barrier(jnp.sum(jnp.exp(logits), axis=-1, keepdims=True)))
    q_taken = lax.optimization_barrier(jnp.sum(onehot_f * qvalues, axis=-1))
    value_term = 0.5 * (q_taken - targets) ** 2
    policy_term = -taken_weight * lax.optimization_barrier(jnp.sum(onehot_f * logpol, axis=-1))
    regular = -lax.optimization_barrier(jnp.sum(cmpo_policy * logpol, axis=-1))
    return jnp.sum(value_term + policy_term + regular) * norm_scale

def backward(cotangent, rounded, squashed, onehot, w_hidden, w_heads):
    unroll_len = len(squashed)
    hid = w_hidden.shape[0]
    grad_state = jnp.zeros(squashed[0].shape, jnp.float32)
    grad_hidden = jnp.zeros((hid, hid), jnp.float32)
    grad_action = jnp.zeros((hid, onehot.shape[-1]), jnp.float32)
    grad_heads = jnp.zeros(w_heads.shape, jnp.float32)
    for step in range(unroll_len - 1, -1, -1):
        grad_pre = (grad_state * (1.0 - squashed[step] * squashed[step])).astype(jnp.bfloat16)
        head_cot = cotangent[step].astype(jnp.bfloat16)
        grad_hidden = grad_hidden + jnp.dot(rounded[step].T, grad_pre, preferred_element_type=jnp.float32)
        grad_action = grad_action + jnp.dot(grad_pre.T, onehot[:, step], preferred_element_type=jnp.float32)
        grad_heads = grad_heads + jnp.dot(rounded[step].T, head_cot, preferred_element_type=jnp.float32)
        grad_state = grad_state + jnp.dot(grad_pre, w_hidden.T, preferred_element_type=jnp.float32)
        grad_state = grad_state + jnp.dot(head_cot, w_heads.T, preferred_element_type=jnp.float32)
    return (grad_hidden, grad_action, grad_heads)

def reference(embed, actions, rewards, ends, behaviour, w_hidden, w_action, w_heads):
    emb_blocks = embed.reshape(DEVICES, B_DEV, HID)
    act_blocks = actions.reshape(DEVICES, B_DEV, STEPS)

    def heads_of(inputs):
        return unroll(inputs[0], inputs[1], w_hidden, w_action, w_heads)[0]
    head_out = lax.map(heads_of, (emb_blocks, act_blocks))
    head_out = jnp.transpose(head_out, (1, 0, 2, 3)).reshape(STEPS + 1, TOTAL, 2 * ACTIONS)
    policy, onehot_f, targets, advantage = estimates(head_out, actions, rewards, ends, behaviour)
    grouped = advantage.reshape(STEPS, N_REP, N_BATCH * B_DEV, ACTIONS)
    spread = lax.optimization_barrier(jnp.sum(grouped * grouped, axis=(0, 2, 3)))
    spread_scale = jnp.sqrt(spread / (N_BATCH * B_DEV * STEPS * ACTIONS) + EPSILON)
    scale_rows = jnp.repeat(spread_scale, N_BATCH * B_DEV, total_repeat_length=TOTAL)
    weights = jnp.exp(jnp.clip(advantage / scale_rows[None, :, None], -1.0, 1.0))
    norm_mass = lax.optimization_barrier(jnp.sum(policy * weights, axis=-1))
    mass_sum = lax.optimization_barrier(jnp.sum(norm_mass.reshape(STEPS, N_REP, N_BATCH * B_DEV), axis=(0, 2)))
    mean_mass = mass_sum / (N_BATCH * B_DEV * STEPS)
    mass_rows = jnp.repeat(mean_mass, N_BATCH * B_DEV, total_repeat_length=TOTAL)
    cmpo_policy = policy * weights / norm_mass[:, :, None]
    taken_weight = lax.optimization_barrier(jnp.sum(onehot_f * weights, axis=-1)) / mass_rows[None, :]
    cotangent = jax.grad(objective)(head_out, onehot_f, targets, cmpo_policy, taken_weight, 1.0 / (TOTAL * STEPS))
    cot_blocks = jnp.transpose(cotangent.reshape(STEPS + 1, DEVICES, B_DEV, 2 * ACTIONS), (1, 0, 2, 3))

    def accumulate(sums_acc, inputs):
        _, rounded, squashed, onehot = unroll(inputs[0], inputs[1], w_hidden, w_action, w_heads)
        partial_value = backward(inputs[2], rounded, squashed, onehot, w_hidden, w_heads)
        return ((sums_acc[0] + partial_value[0], sums_acc[1] + partial_value[1], sums_acc[2] + partial_value[2]), None)
    zero_sums = (jnp.zeros((HID, HID), jnp.float32), jnp.zeros((HID, ACTIONS), jnp.float32), jnp.zeros((HID, 2 * ACTIONS), jnp.float32))
    summed, _ = lax.scan(accumulate, zero_sums, (emb_blocks, act_blocks, cot_blocks))
    return (summed[0], summed[1].T, summed[2], targets.T)
```

```python
import jax
import jax.numpy as jnp
from jax import lax
from jax.experimental import pallas as pl
from jax.experimental.pallas import tpu as pltpu
from jax.sharding import Mesh
from jax.sharding import PartitionSpec as P

ALL = ("z", "x", "core", "y")
PLANE = ("x", "y")

DISCOUNT = 0.997
TRACE_LAMBDA = 0.95
EPSILON = 1e-06

LANES = 128
F32 = jnp.float32
BF16 = jnp.bfloat16

VMEM = pl.BlockSpec(memory_space=pltpu.VMEM)
SMEM = pl.BlockSpec(memory_space=pltpu.SMEM)


def dot(a, b):
    return jnp.dot(a, b, preferred_element_type=F32)


def dot_nt(a, b):
    return lax.dot_general(a, b, (((1,), (1,)), ((), ())), preferred_element_type=F32)


def dot_tn(a, b):
    return lax.dot_general(a, b, (((0,), (0,)), ((), ())), preferred_element_type=F32)


def kernel_call(body, outs, inputs, scratch=(), scalars=0):
    return pl.pallas_call(
        body,
        out_shape=tuple(jax.ShapeDtypeStruct(s, d) for s, d in outs),
        in_specs=[SMEM] * scalars + [VMEM] * (len(inputs) - scalars),
        out_specs=tuple(VMEM for _ in outs),
        scratch_shapes=list(scratch),
        name=body.__name__,
        compiler_params=pltpu.CompilerParams(vmem_limit_bytes=48 * 1024 * 1024),
    )(*inputs)


def lanes_of(rows):
    return lax.broadcasted_iota(jnp.int32, (rows, LANES), 1)


def onehot_of(act_ref, step):
    rows = act_ref.shape[0]
    return lanes_of(rows) == act_ref[:, step : step + 1]


def pad_rows(dst, src):
    dst[...] = jnp.zeros_like(dst)
    dst[: src.shape[0], :] = src[...]


def pad_lanes(dst, src):
    dst[...] = jnp.zeros_like(dst)
    dst[:, : src.shape[1]] = src[...]


def policy_of(out, count):
    valid = lanes_of(out.shape[0]) < count
    q = jnp.where(valid, pltpu.roll(out, LANES - count, 1), 0.0)
    logits = jnp.where(valid, out, 0.0)
    e = jnp.where(valid, jnp.exp(logits), 0.0)
    total = jnp.sum(e, axis=1, keepdims=True)
    pi = e / total
    v = jnp.sum(pi * q, axis=1, keepdims=True)
    return valid, logits, q, pi, total, v


def unroll_kernel(emb, act, wh, wa, whd, s_out, t_out, st_out, o_out, ssq_out, wap, whp):
    count = wa.shape[0]
    steps = act.shape[1]
    rows = emb.shape[0]
    pad_rows(wap, wa)
    pad_lanes(whp, whd)
    state = emb[...].astype(F32)
    for k in range(steps):
        s = state.astype(BF16)
        s_out[k * rows : (k + 1) * rows, :] = s
        if k < steps - 1:
            oh = onehot_of(act, k).astype(F32).astype(BF16)
            t = jnp.tanh(dot(s, wh[...]) + dot(oh, wap[...]))
            t_out[k * rows : (k + 1) * rows, :] = t
            state = state + t
    st_out[...] = state
    out = dot(s_out[...], whp[...])
    o_out[...] = out
    valid, _, q, _, _, v = policy_of(out, count)
    adv = jnp.where(valid, q - v, 0.0)
    part = jnp.sum(jnp.sum(adv * adv, axis=0, keepdims=True), axis=1, keepdims=True)
    ssq_out[...] = jnp.broadcast_to(part, ssq_out.shape)


def targets_kernel(act, rew, ends, beh, wh, wa, whd, s, st, o, tg_out, sT_out, wap, whp):
    count = wa.shape[0]
    steps = act.shape[1]
    rows = st.shape[0]
    pad_rows(wap, wa)
    pad_lanes(whp, whd)
    last = steps - 1
    oh = onehot_of(act, last).astype(F32).astype(BF16)
    t = jnp.tanh(dot(s[last * rows :, :], wh[...]) + dot(oh, wap[...]))
    final = (st[...] + t).astype(BF16)
    v_next = policy_of(dot(final, whp[...]), count)[-1]
    lane = lanes_of(rows)
    carried = jnp.zeros((rows, 1), F32)
    tg = jnp.zeros((rows, LANES), F32)
    for k in range(last, -1, -1):
        valid, logits, _, _, total, v = policy_of(o[k * rows : (k + 1) * rows, :], count)
        b = beh[k * rows : (k + 1) * rows, :]
        b_total = jnp.sum(jnp.where(valid, jnp.exp(b), 0.0), axis=1, keepdims=True)
        gap = (logits - jnp.log(total)) - (b - jnp.log(b_total))
        ratio = jnp.exp(jnp.sum(jnp.where(onehot_of(act, k), gap, 0.0), axis=1, keepdims=True))
        clipped = jnp.minimum(1.0, ratio)
        open_ = 1.0 - ends[:, k : k + 1].astype(F32)
        td = rew[:, k : k + 1] + DISCOUNT * open_ * v_next - v
        carried = clipped * td + DISCOUNT * TRACE_LAMBDA * open_ * clipped * carried
        tg = jnp.where(lane == k, v + carried, tg)
        v_next = v
    tg_out[...] = tg[:, :steps]
    for k in range(steps):
        sT_out[:, k * rows : (k + 1) * rows] = s[k * rows : (k + 1) * rows, :].T


def weights_kernel(groups, devices, act, o, tg, ssq0, ssq1, ssq2, ssq3, a_out, b_out, mass_out):
    steps = act.shape[1]
    rows = act.shape[0]
    count = ACTIONS
    spread = ssq0[0:1, 0:1] + ssq1[0:1, 0:1] + ssq2[0:1, 0:1] + ssq3[0:1, 0:1]
    scale = jnp.sqrt(spread / (groups * rows * steps * count) + EPSILON)
    norm = 1.0 / (devices * rows * steps)
    mass_sum = jnp.zeros((1, 1), F32)
    for k in range(steps):
        valid, _, q, pi, _, v = policy_of(o[k * rows : (k + 1) * rows, :], count)
        oh = onehot_of(act, k)
        w = jnp.exp(jnp.clip((q - v) / scale, -1.0, 1.0))
        pw = pi * w
        mass = jnp.sum(pw, axis=1, keepdims=True)
        mass_sum = mass_sum + jnp.sum(mass, axis=0, keepdims=True)
        cmpo = pw / mass
        whole = jnp.sum(cmpo, axis=1, keepdims=True)
        taken = jnp.sum(jnp.where(oh, w, 0.0), axis=1, keepdims=True)
        dq = jnp.where(oh, q - tg[:, k : k + 1], 0.0)
        a = (pi * whole - cmpo) + pltpu.roll(dq, count, 1)
        b = taken * (pi - jnp.where(oh, 1.0, 0.0))
        a_out[k * rows : (k + 1) * rows, :] = a * norm
        b_out[k * rows : (k + 1) * rows, :] = b * norm
    mass_out[...] = jnp.broadcast_to(mass_sum, mass_out.shape)


def gradient_kernel(
    groups, core, act, a, b, m0, m1, m2, m3, s, sT, t, wh, whd, mine, other, whp, g, x, oh, e
):
    steps = act.shape[1]
    rows = act.shape[0]
    pad_lanes(whp, whd)
    total = m0[0:1, 0:1] + m1[0:1, 0:1] + m2[0:1, 0:1] + m3[0:1, 0:1]
    mean = total / (groups * rows * steps)
    g[...] = (a[...] + b[...] / mean).astype(BF16)
    last = steps - 1
    r = dot_nt(g[last * rows :, :], whp[...])
    for k in range(last - 1, -1, -1):
        here = slice(k * rows, (k + 1) * rows)
        tk = t[here, :]
        xk = (r * (1.0 - tk * tk)).astype(BF16)
        x[here, :] = xk
        oh[here, :] = onehot_of(act, k).astype(F32).astype(BF16)
        if k > 0:
            r = r + (dot_nt(xk, wh[...]) + dot_nt(g[here, :], whp[...]))
    inner = last * rows
    heads = dot_tn(g[...], s[...])
    taken = dot_tn(oh[...], x[...])
    e[0:40, :] = heads[0:40, :]
    e[40:64, :] = taken[0:24, :]
    hid = sT.shape[0]
    half = hid // 2
    units = mine.shape[0]
    which = core[0]
    for out, h in ((other, 1 - which), (mine, which)):
        at = pl.multiple_of(h * half, half)
        left = sT[pl.ds(at, half), :inner]
        for j in range(0, hid, 256):
            block = dot(left, x[:, j : j + 256])
            for c in range(2):
                n = j // LANES + c
                out[:, n * 32 : (n + 1) * 32, :] = block[:, c * LANES : (c + 1) * LANES].reshape(
                    units, 32, LANES
                )
        for i in range(4):
            rows8 = e[pl.ds(pl.multiple_of(h * 32 + i * 8, 8), 8), :]
            for n in range(8):
                at8 = 256 + (n % 2) * 8
                out[i * 4 + n // 2, at8 : at8 + 8, :] = rows8[:, n * LANES : (n + 1) * LANES]


def plane_sum_kernel(arrived, out):
    total = arrived[0]
    for i in range(1, arrived.shape[0]):
        total = total + arrived[i]
    out[...] = jnp.zeros_like(out)
    for n in range(8):
        out[n, 0:32, :] = total[n * 32 : (n + 1) * 32, :]
        out[n, 32:34, :] = total[256 + n * 2 : 258 + n * 2, :]


def line_sum_kernel(arrived, out):
    total = arrived[0]
    for i in range(1, arrived.shape[0]):
        total = total + arrived[i]
    for i in range(out.shape[0]):
        out[i] = total


def unpack_kernel(arrived, out, unit):
    for n in range(8):
        unit[n * 32 : (n + 1) * 32, :] = arrived[n, 0:32, :]
        unit[256 + n * 2 : 258 + n * 2, :] = arrived[n, 32:34, :]
    whole = unit[...]
    for i in range(out.shape[0]):
        out[i] = whole


def assemble_kernel(core, mine, other, gh, ga, gd, e):
    half = gh.shape[0] // 2
    which = core[0]
    for part, h in ((mine, which), (other, 1 - which)):
        at = pl.multiple_of(h * half, half)
        for n in range(8):
            gh[pl.ds(at, half), n * LANES : (n + 1) * LANES] = part[
                :, n * 32 : (n + 1) * 32, :
            ].reshape(half, LANES)
        for i in range(4):
            for n in range(8):
                at8 = 256 + (n % 2) * 8
                e[pl.ds(pl.multiple_of(h * 32 + i * 8, 8), 8), n * LANES : (n + 1) * LANES] = part[
                    i * 4 + n // 2, at8 : at8 + 8, :
                ]
    ga[...] = e[40 : 40 + ga.shape[0], :]
    gd[...] = e[0:40, :].T[:, : gd.shape[1]]


ACTIONS = 18


def shifted(array, axis, by):
    size = lax.axis_size(axis)
    return lax.ppermute(array, axis, [(i, (i + by) % size) for i in range(size)])


def of_group(part):
    return [part] + [shifted(part, "y", by) for by in (2, 1, 3)]


def swapped(tiles, axis):
    return lax.all_to_all(tiles, axis, split_axis=0, concat_axis=0, tiled=True)


def body(embed, actions, rewards, ends, behaviour, w_hidden, w_action, w_heads):
    rows, hid = embed.shape
    steps = actions.shape[1]
    groups = lax.axis_size("y")
    devices = lax.axis_size(ALL)
    core = lax.axis_index("core").astype(jnp.int32).reshape(1)

    wap = pltpu.VMEM((LANES, hid), BF16)
    whp = pltpu.VMEM((hid, LANES), BF16)
    s, t, state, out, ssq = kernel_call(
        unroll_kernel,
        [
            ((steps * rows, hid), BF16),
            (((steps - 1) * rows, hid), F32),
            ((rows, hid), F32),
            ((steps * rows, LANES), F32),
            ((8, LANES), F32),
        ],
        (embed, actions, w_hidden, w_action, w_heads),
        (wap, whp),
    )
    ssqs = of_group(ssq)
    beh = jnp.pad(
        jnp.transpose(behaviour, (1, 0, 2)), ((0, 0), (0, 0), (0, LANES - behaviour.shape[2]))
    ).reshape(steps * rows, LANES)
    targets, sT = kernel_call(
        targets_kernel,
        [((rows, steps), F32), ((hid, steps * rows), BF16)],
        (actions, rewards, ends, beh, w_hidden, w_action, w_heads, s, state, out),
        (wap, whp),
    )

    def weights_body(*refs):
        weights_kernel(groups, devices, *refs)

    a, b, mass = kernel_call(
        weights_body,
        [((steps * rows, LANES), F32), ((steps * rows, LANES), F32), ((8, LANES), F32)],
        (actions, out, targets, *ssqs),
    )
    masses = of_group(mass)

    def gradient_body(*refs):
        gradient_kernel(groups, *refs)

    unit = ((16, 272, LANES), F32)
    mine, other = kernel_call(
        gradient_body,
        [unit, unit],
        (core, actions, a, b, *masses, s, sT, t, w_hidden, w_heads),
        (
            whp,
            pltpu.VMEM((steps * rows, LANES), BF16),
            pltpu.VMEM(((steps - 1) * rows, hid), BF16),
            pltpu.VMEM(((steps - 1) * rows, LANES), BF16),
            pltpu.VMEM((64, hid), F32),
        ),
        scalars=1,
    )
    chip = mine + shifted(other, "core", 1)
    (line,) = kernel_call(plane_sum_kernel, [((8, 40, LANES), F32)], (swapped(chip, PLANE),))
    (total,) = kernel_call(line_sum_kernel, [((8, 40, LANES), F32)], (swapped(line, "z"),))
    (plane,) = kernel_call(
        unpack_kernel, [unit], (swapped(total, "z"),), (pltpu.VMEM((272, LANES), F32),)
    )
    mine = swapped(plane, PLANE)
    other = shifted(mine, "core", 1)
    grad_hidden, grad_action, grad_heads = kernel_call(
        assemble_kernel,
        [((hid, hid), F32), (w_action.shape, F32), (w_heads.shape, F32)],
        (core, mine, other),
        (pltpu.VMEM((64, hid), F32),),
        scalars=1,
    )
    return (grad_hidden, grad_action, grad_heads, targets)


def solution(mesh):
    torus = Mesh(mesh.devices.reshape(8, 4, 2, mesh.shape["batch"]), ALL)
    return jax.shard_map(
        body,
        mesh=torus,
        in_specs=(
            P(ALL, None),
            P(ALL, None),
            P(ALL, None),
            P(ALL, None),
            P(ALL, None, None),
            P(),
            P(),
            P(),
        ),
        out_specs=(P(), P(), P(), P(ALL, None)),
        check_vma=False,
    )
```

```python
import jax
import jax.numpy as jnp
from jax import lax
from jax.experimental import pallas as pl
from jax.experimental.pallas import tpu as pltpu
from jax.sharding import Mesh
from jax.sharding import PartitionSpec as P

ALL = ("zh", "zp", "x", "core", "y")
NEAR = ("zp", "x", "y")
LINE = ("zh", "zp")

DISCOUNT = 0.997
TRACE_LAMBDA = 0.95
EPSILON = 1e-06

LANES = 128
Q_ROW = 24
A_ROW = 40
F32 = jnp.float32
BF16 = jnp.bfloat16

VMEM = pl.BlockSpec(memory_space=pltpu.VMEM)
SMEM = pl.BlockSpec(memory_space=pltpu.SMEM)


def dot(a, b):
    return jnp.dot(a, b, preferred_element_type=F32)


def dot_nt(a, b):
    return lax.dot_general(a, b, (((1,), (1,)), ((), ())), preferred_element_type=F32)


def dot_tn(a, b):
    return lax.dot_general(a, b, (((0,), (0,)), ((), ())), preferred_element_type=F32)


def kernel_call(body, outs, inputs, scratch=(), scalars=0):
    return pl.pallas_call(
        body,
        out_shape=tuple(jax.ShapeDtypeStruct(s, d) for s, d in outs),
        in_specs=[SMEM] * scalars + [VMEM] * (len(inputs) - scalars),
        out_specs=tuple(VMEM for _ in outs),
        scratch_shapes=list(scratch),
        name=body.__name__,
        compiler_params=pltpu.CompilerParams(vmem_limit_bytes=12 * 1024 * 1024),
    )(*inputs)


def chosen(act, step, count):
    columns = act.shape[1]
    return lax.broadcasted_iota(jnp.int32, (count, columns), 0) == act[step : step + 1, :]


def onehot_of(act, step):
    return chosen(act, step, 32).astype(F32).astype(BF16)


def policy_of(out, at, count):
    logits = out[0:count, at]
    q = out[Q_ROW : Q_ROW + count, at]
    e = jnp.exp(logits)
    total = jnp.sum(e, axis=0, keepdims=True)
    pi = e / total
    v = jnp.sum(pi * q, axis=0, keepdims=True)
    return logits, q, pi, total, v


def unroll_kernel(emb, act, wh, wa, whd, s_out, t_out, st_out, o_out, ssq_out, wap, whp, wide, rows40):
    count = wa.shape[0]
    steps = act.shape[0]
    rows = emb.shape[0]
    wap[...] = jnp.zeros_like(wap)
    wap[:count, :] = wa[...]
    rows40[0 : 2 * count, :] = whd[...].astype(F32)
    wide[...] = jnp.zeros_like(wide)
    wide[0:count, :] = rows40[0:count, :]
    wide[Q_ROW : Q_ROW + count, :] = rows40[count : 2 * count, :]
    whp[...] = wide[...].astype(BF16)
    state = emb[...].astype(F32)
    for k in range(steps):
        s = state.astype(BF16)
        s_out[k * rows : (k + 1) * rows, :] = s
        if k < steps - 1:
            t = jnp.tanh(dot(s, wh[...]) + dot_tn(onehot_of(act, k), wap[...]))
            t_out[k * rows : (k + 1) * rows, :] = t
            state = state + t
    st_out[...] = state
    o_out[...] = dot_nt(whp[...], s_out[...])
    _, q, _, _, v = policy_of(o_out, slice(None), count)
    adv = q - v
    part = jnp.sum(jnp.sum(adv * adv, axis=1, keepdims=True), axis=0, keepdims=True)
    ssq_out[...] = jnp.broadcast_to(part, ssq_out.shape)


def targets_kernel(act, rew, ends, beh, wh, wap, whp, s, st, o, tg_out, sT_out, last_out):
    steps = act.shape[0]
    rows = st.shape[0]
    count = beh.shape[1]
    last = steps - 1
    t = jnp.tanh(dot(s[last * rows :, :], wh[...]) + dot_tn(onehot_of(act, last), wap[...]))
    last_out[...] = dot_nt(whp[...], (st[...] + t).astype(BF16))
    v_next = policy_of(last_out, slice(None), count)[-1]
    carried = jnp.zeros((1, rows), F32)
    for k in range(last, -1, -1):
        logits, _, _, total, v = policy_of(o, slice(k * rows, (k + 1) * rows), count)
        b = beh[k]
        b_total = jnp.sum(jnp.exp(b), axis=0, keepdims=True)
        gap = (logits - jnp.log(total)) - (b - jnp.log(b_total))
        ratio = jnp.exp(jnp.sum(jnp.where(chosen(act, k, count), gap, 0.0), axis=0, keepdims=True))
        clipped = jnp.minimum(1.0, ratio)
        open_ = 1.0 - ends[k : k + 1, :].astype(F32)
        td = rew[k : k + 1, :] + DISCOUNT * open_ * v_next - v
        carried = clipped * td + DISCOUNT * TRACE_LAMBDA * open_ * clipped * carried
        tg_out[k : k + 1, :] = v + carried
        v_next = v
    for k in range(steps):
        sT_out[:, k * rows : (k + 1) * rows] = s[k * rows : (k + 1) * rows, :].T


def weights_kernel(groups, devices, count, act, o, tg, ssq0, ssq1, ssq2, ssq3, a_out, b_out, mass_out):
    steps, rows = act.shape
    spread = ssq0[0:1, 0:1] + ssq1[0:1, 0:1] + ssq2[0:1, 0:1] + ssq3[0:1, 0:1]
    scale = jnp.sqrt(spread / (groups * rows * steps * count) + EPSILON)
    norm = 1.0 / (devices * rows * steps)
    mass_sum = jnp.zeros((1, rows), F32)
    a_out[...] = jnp.zeros_like(a_out)
    b_out[...] = jnp.zeros_like(b_out)
    for k in range(steps):
        at = slice(k * rows, (k + 1) * rows)
        _, q, pi, _, v = policy_of(o, at, count)
        oh = chosen(act, k, count)
        w = jnp.exp(jnp.clip((q - v) / scale, -1.0, 1.0))
        pw = pi * w
        mass = jnp.sum(pw, axis=0, keepdims=True)
        mass_sum = mass_sum + mass
        cmpo = pw / mass
        whole = jnp.sum(cmpo, axis=0, keepdims=True)
        taken = jnp.sum(jnp.where(oh, w, 0.0), axis=0, keepdims=True)
        a_out[0:count, at] = (pi * whole - cmpo) * norm
        a_out[Q_ROW : Q_ROW + count, at] = jnp.where(oh, q - tg[k : k + 1, :], 0.0) * norm
        b_out[0:count, at] = taken * (pi - jnp.where(oh, 1.0, 0.0)) * norm
    mass_out[...] = jnp.broadcast_to(jnp.sum(mass_sum, axis=1, keepdims=True), mass_out.shape)


def gradient_kernel(
    groups, count, place, act, a, b, m0, m1, m2, m3, s, sT, t, wh, whp, mine, other, gf, g, x, oh, e
):
    steps, rows = act.shape
    total = m0[0:1, 0:1] + m1[0:1, 0:1] + m2[0:1, 0:1] + m3[0:1, 0:1]
    mean = total / (groups * rows * steps)
    gf[...] = a[...]
    gf[0:Q_ROW, :] = a[0:Q_ROW, :] + b[...] / mean
    g[...] = gf[...].astype(BF16)
    last = steps - 1
    r = dot_tn(g[:, last * rows :], whp[...])
    for k in range(last - 1, -1, -1):
        here = slice(k * rows, (k + 1) * rows)
        tk = t[here, :]
        xk = (r * (1.0 - tk * tk)).astype(BF16)
        x[here, :] = xk
        oh[:, here] = onehot_of(act, k)
        if k > 0:
            r = r + (dot_nt(xk, wh[...]) + dot_tn(g[:, here], whp[...]))
    inner = last * rows
    e[...] = jnp.zeros_like(e)
    heads = dot(g[...], s[...])
    e[0:count, :] = heads[0:count, :]
    e[count : 2 * count, :] = heads[Q_ROW : Q_ROW + count, :]
    e[A_ROW : A_ROW + count, :] = dot(oh[...], x[...])[0:count, :]
    hid = sT.shape[0]
    half = hid // 2
    core, flip = place[0], place[1]
    for out, h in ((other, 1 - core), (mine, core)):
        left = sT[pl.ds(pl.multiple_of(h * half, half), half), :inner]
        for j in range(0, hid, 256):
            block = dot(left, x[:, j : j + 256])
            for p in range(2):
                slot = pl.ds((flip + p - 2 * flip * p) * 16, 16)
                for c in range(2):
                    n = j // LANES + c
                    out[slot, n * 16 : (n + 1) * 16, :] = block[
                        p * 256 : (p + 1) * 256, c * LANES : (c + 1) * LANES
                    ].reshape(16, 16, LANES)
        for i in range(4):
            p = i // 2
            slot = (flip + p - 2 * flip * p) * 16 + (i % 2) * 8
            rows8 = e[pl.ds(pl.multiple_of(h * 32 + i * 8, 8), 8), :]
            for n in range(8):
                out[slot + n, 128:136, :] = rows8[:, n * LANES : (n + 1) * LANES]


def plane_sum_kernel(arrived, out):
    total = arrived[0]
    for i in range(1, arrived.shape[0]):
        total = total + arrived[i]
    out[...] = total


def line_sum_kernel(own, near, far, both, out):
    total = (own[...] + near[...]) + (far[...] + both[...])
    for i in range(out.shape[0]):
        out[i] = total


def assemble_kernel(place, mine, other, gh, ga, gd, e):
    half = gh.shape[0] // 2
    core, flip = place[0], place[1]
    for part, h in ((mine, core), (other, 1 - core)):
        for p in range(2):
            slot = pl.ds((flip + p - 2 * flip * p) * 16, 16)
            at = pl.ds(pl.multiple_of(h * half + p * 256, 256), 256)
            for n in range(8):
                gh[at, n * LANES : (n + 1) * LANES] = part[
                    slot, n * 16 : (n + 1) * 16, :
                ].reshape(256, LANES)
        for i in range(4):
            p = i // 2
            slot = (flip + p - 2 * flip * p) * 16 + (i % 2) * 8
            at8 = pl.ds(pl.multiple_of(h * 32 + i * 8, 8), 8)
            for n in range(8):
                e[at8, n * LANES : (n + 1) * LANES] = part[slot + n, 128:136, :]
    ga[...] = e[A_ROW : A_ROW + ga.shape[0], :]
    gd[...] = e[0 : gd.shape[0], :]


def shifted(array, axis, by):
    size = lax.axis_size(axis)
    return lax.ppermute(array, axis, [(i, (i + by) % size) for i in range(size)])


def of_group(part):
    return [part] + [shifted(part, "y", by) for by in (2, 1, 3)]


def swapped(tiles, axis):
    return lax.all_to_all(tiles, axis, split_axis=0, concat_axis=0, tiled=True)


def along_z(array, to):
    return lax.ppermute(array, LINE, [(z, to(z)) for z in range(8)])


def beside(z):
    return (z + 1 if z % 2 else z - 1) % 8


def across(z):
    return (z + 4) % 8


def body(embed, actions, rewards, ends, behaviour, w_hidden, w_action, w_heads):
    rows, hid = embed.shape
    steps = actions.shape[1]
    count = w_action.shape[0]
    groups = lax.axis_size("y")
    devices = lax.axis_size(ALL)
    place = jnp.stack([lax.axis_index("core"), lax.axis_index("zh") % 2]).astype(jnp.int32)
    act = actions.T

    s, t, state, out, ssq, wap, whp = kernel_call(
        unroll_kernel,
        [
            ((steps * rows, hid), BF16),
            (((steps - 1) * rows, hid), F32),
            ((rows, hid), F32),
            ((48, steps * rows), F32),
            ((8, LANES), F32),
            ((32, hid), BF16),
            ((48, hid), BF16),
        ],
        (embed, act, w_hidden, w_action, w_heads.T),
        (pltpu.VMEM((48, hid), F32), pltpu.VMEM((40, hid), F32)),
    )
    ssqs = of_group(ssq)
    targets, sT = kernel_call(
        targets_kernel,
        [((steps, rows), F32), ((hid, steps * rows), BF16)],
        (
            act,
            rewards.T,
            ends.T,
            jnp.transpose(behaviour, (1, 2, 0)),
            w_hidden,
            wap,
            whp,
            s,
            state,
            out,
        ),
        (pltpu.VMEM((48, rows), F32),),
    )

    def weights_body(*refs):
        weights_kernel(groups, devices, count, *refs)

    a, b, mass = kernel_call(
        weights_body,
        [((48, steps * rows), F32), ((Q_ROW, steps * rows), F32), ((8, LANES), F32)],
        (act, out, targets, *ssqs),
    )
    masses = of_group(mass)

    def gradient_body(*refs):
        gradient_kernel(groups, count, *refs)

    parts = ((32, 136, LANES), F32)
    mine, other = kernel_call(
        gradient_body,
        [parts, parts],
        (place, act, a, b, *masses, s, sT, t, w_hidden, whp),
        (
            pltpu.VMEM((48, steps * rows), F32),
            pltpu.VMEM((48, steps * rows), BF16),
            pltpu.VMEM(((steps - 1) * rows, hid), BF16),
            pltpu.VMEM((32, (steps - 1) * rows), BF16),
            pltpu.VMEM((64, hid), F32),
        ),
        scalars=1,
    )
    chip = mine + shifted(other, "core", 1)
    (own,) = kernel_call(plane_sum_kernel, [((136, LANES), F32)], (swapped(chip, NEAR),))
    far = along_z(own, across)
    both = along_z(own, lambda z: across(beside(z)))
    near = along_z(own, beside)
    (whole,) = kernel_call(line_sum_kernel, [parts], (own, near, far, both))
    mine = swapped(whole, NEAR)
    other = shifted(mine, "core", 1)
    grad_hidden, grad_action, grad_heads = kernel_call(
        assemble_kernel,
        [((hid, hid), F32), (w_action.shape, F32), (w_heads.shape[::-1], F32)],
        (place, mine, other),
        (pltpu.VMEM((64, hid), F32),),
        scalars=1,
    )
    return (grad_hidden, grad_action, grad_heads.T, targets.T)


def solution(mesh):
    torus = Mesh(mesh.devices.reshape(4, 2, 4, 2, mesh.shape["batch"]), ALL)
    return jax.shard_map(
        body,
        mesh=torus,
        in_specs=(
            P(ALL, None),
            P(ALL, None),
            P(ALL, None),
            P(ALL, None),
            P(ALL, None, None),
            P(),
            P(),
            P(),
        ),
        out_specs=(P(), P(), P(), P(ALL, None)),
        check_vma=False,
    )
```

```python
import jax
import jax.numpy as jnp
from jax import lax
from jax.experimental import pallas as pl
from jax.experimental.pallas import tpu as pltpu
from jax.sharding import Mesh
from jax.sharding import PartitionSpec as P

ALL = ("zh", "zp", "x", "core", "y")
NEAR = ("zp", "x", "y")
LINE = ("zh", "zp")

DISCOUNT = 0.997
TRACE_LAMBDA = 0.95
EPSILON = 1e-06

LANES = 128
Q_ROW = 24
A_ROW = 40
F32 = jnp.float32
BF16 = jnp.bfloat16

VMEM = pl.BlockSpec(memory_space=pltpu.VMEM)
SMEM = pl.BlockSpec(memory_space=pltpu.SMEM)
HBM = pl.BlockSpec(memory_space=pltpu.MemorySpace.HBM)


def dot(a, b):
    return jnp.dot(a, b, preferred_element_type=F32)


def dot_nt(a, b):
    return lax.dot_general(a, b, (((1,), (1,)), ((), ())), preferred_element_type=F32)


def dot_tn(a, b):
    return lax.dot_general(a, b, (((0,), (0,)), ((), ())), preferred_element_type=F32)


def kernel_call(body, outs, inputs, scratch=(), scalars=0, far=(), far_outs=(), aliases=None):
    return pl.pallas_call(
        body,
        out_shape=tuple(jax.ShapeDtypeStruct(s, d) for s, d in outs),
        in_specs=[
            SMEM if i < scalars else HBM if i in far else VMEM for i in range(len(inputs))
        ],
        out_specs=tuple(HBM if i in far_outs else VMEM for i in range(len(outs))),
        scratch_shapes=list(scratch),
        input_output_aliases=aliases or {},
        name=body.__name__,
        compiler_params=pltpu.CompilerParams(vmem_limit_bytes=16 * 1024 * 1024),
    )(*inputs)


def started(source, target, sem):
    copy = pltpu.make_async_copy(source, target, sem)
    copy.start()
    return copy


def chosen(act, step, count):
    columns = act.shape[1]
    return lax.broadcasted_iota(jnp.int32, (count, columns), 0) == act[step : step + 1, :]


def onehot_of(act, step):
    return chosen(act, step, 32).astype(F32).astype(BF16)


def policy_of(out, at, count):
    logits = out[0:count, at]
    q = out[Q_ROW : Q_ROW + count, at]
    e = jnp.exp(logits)
    total = jnp.sum(e, axis=0, keepdims=True)
    pi = e / total
    v = jnp.sum(pi * q, axis=0, keepdims=True)
    return logits, q, pi, total, v


def unroll_kernel(
    emb_far, act_far, wh_far, wa_far, whd_far,
    s_out, t_far, o_out, ssq_out, act, whp,
    emb, wh, wa, whd, t_buf, wap, wide, rows40, sem, t_sem,
):
    loads = [
        started(source, target, sem.at[i])
        for i, (source, target) in enumerate(
            ((wh_far, wh), (emb_far, emb), (act_far, act), (wa_far, wa), (whd_far, whd))
        )
    ]
    count = wa.shape[0]
    steps = act.shape[0]
    rows = emb.shape[0]
    wap[...] = jnp.zeros_like(wap)
    wide[...] = jnp.zeros_like(wide)
    for load in loads[1:]:
        load.wait()
    wap[:count, :] = wa[...]
    rows40[0 : 2 * count, :] = whd[...].astype(F32)
    wide[0:count, :] = rows40[0:count, :]
    wide[Q_ROW : Q_ROW + count, :] = rows40[count : 2 * count, :]
    whp[...] = wide[...].astype(BF16)
    state = emb[...].astype(F32)
    loads[0].wait()
    stores = []
    for k in range(steps):
        here = slice(k * rows, (k + 1) * rows)
        s = state.astype(BF16)
        s_out[here, :] = s
        t = jnp.tanh(dot(s, wh[...]) + dot_tn(onehot_of(act, k), wap[...]))
        if k < steps - 1:
            t_buf[here, :] = t
            stores.append(started(t_buf.at[here, :], t_far.at[here, :], t_sem.at[k]))
        state = state + t
    inner = steps * rows
    o_out[:, :inner] = dot_nt(whp[...], s_out[...])
    o_out[:, inner:] = dot_nt(whp[...], state.astype(BF16))
    _, q, _, _, v = policy_of(o_out, slice(0, inner), count)
    adv = q - v
    part = jnp.sum(jnp.sum(adv * adv, axis=1, keepdims=True), axis=0, keepdims=True)
    ssq_out[...] = jnp.broadcast_to(part, ssq_out.shape)
    for store in stores:
        store.wait()


def targets_kernel(rew_far, ends_far, beh_far, act, s, o, tg_far, tg_out, sT_out, rew, ends, beh, sem):
    loads = [
        started(source, target, sem.at[i])
        for i, (source, target) in enumerate(((rew_far, rew), (ends_far, ends), (beh_far, beh)))
    ]
    steps, rows = act.shape
    count = beh.shape[1]
    for k in range(steps):
        sT_out[:, k * rows : (k + 1) * rows] = s[k * rows : (k + 1) * rows, :].T
    for load in loads:
        load.wait()
    v_next = policy_of(o, slice(steps * rows, (steps + 1) * rows), count)[-1]
    carried = jnp.zeros((1, rows), F32)
    for k in range(steps - 1, -1, -1):
        logits, _, _, total, v = policy_of(o, slice(k * rows, (k + 1) * rows), count)
        b = beh[k]
        b_total = jnp.sum(jnp.exp(b), axis=0, keepdims=True)
        gap = (logits - jnp.log(total)) - (b - jnp.log(b_total))
        ratio = jnp.exp(jnp.sum(jnp.where(chosen(act, k, count), gap, 0.0), axis=0, keepdims=True))
        clipped = jnp.minimum(1.0, ratio)
        open_ = 1.0 - ends[k : k + 1, :].astype(F32)
        td = rew[k : k + 1, :] + DISCOUNT * open_ * v_next - v
        carried = clipped * td + DISCOUNT * TRACE_LAMBDA * open_ * clipped * carried
        tg_out[k : k + 1, :] = v + carried
        v_next = v
    started(tg_out, tg_far, sem.at[3]).wait()


def weights_kernel(groups, devices, count, act, o, tg, ssq0, ssq1, ssq2, ssq3, a_out, b_out, mass_out):
    steps, rows = act.shape
    spread = ssq0[0:1, 0:1] + ssq1[0:1, 0:1] + ssq2[0:1, 0:1] + ssq3[0:1, 0:1]
    scale = jnp.sqrt(spread / (groups * rows * steps * count) + EPSILON)
    norm = 1.0 / (devices * rows * steps)
    mass_sum = jnp.zeros((1, rows), F32)
    a_out[...] = jnp.zeros_like(a_out)
    b_out[...] = jnp.zeros_like(b_out)
    for k in range(steps):
        at = slice(k * rows, (k + 1) * rows)
        _, q, pi, _, v = policy_of(o, at, count)
        oh = chosen(act, k, count)
        w = jnp.exp(jnp.clip((q - v) / scale, -1.0, 1.0))
        pw = pi * w
        mass = jnp.sum(pw, axis=0, keepdims=True)
        mass_sum = mass_sum + mass
        cmpo = pw / mass
        whole = jnp.sum(cmpo, axis=0, keepdims=True)
        taken = jnp.sum(jnp.where(oh, w, 0.0), axis=0, keepdims=True)
        a_out[0:count, at] = (pi * whole - cmpo) * norm
        a_out[Q_ROW : Q_ROW + count, at] = jnp.where(oh, q - tg[k : k + 1, :], 0.0) * norm
        b_out[0:count, at] = taken * (pi - jnp.where(oh, 1.0, 0.0)) * norm
    mass_out[...] = jnp.broadcast_to(jnp.sum(mass_sum, axis=1, keepdims=True), mass_out.shape)


def gradient_kernel(
    groups, count, place, act, a, b, m0, m1, m2, m3, sT, t_far, wh_far, whp,
    mine, other, gf, g, x, oh, e, t, wh, sem,
):
    steps, rows = act.shape
    last = steps - 1
    spans = [slice(k * rows, (k + 1) * rows) for k in range(steps)]
    loads = {}
    for k in range(last - 1, -1, -1):
        loads[k] = started(t_far.at[spans[k], :], t.at[spans[k], :], sem.at[k])
        if k == last - 1:
            whole = started(wh_far, wh, sem.at[last])
    total = m0[0:1, 0:1] + m1[0:1, 0:1] + m2[0:1, 0:1] + m3[0:1, 0:1]
    mean = total / (groups * rows * steps)
    gf[...] = a[...]
    gf[0:Q_ROW, :] = a[0:Q_ROW, :] + b[...] / mean
    g[...] = gf[...].astype(BF16)
    for k in range(last):
        oh[:, spans[k]] = onehot_of(act, k)
    e[...] = jnp.zeros_like(e)
    heads = dot_nt(g[...], sT[...])
    e[0:count, :] = heads[0:count, :]
    e[count : 2 * count, :] = heads[Q_ROW : Q_ROW + count, :]
    r = dot_tn(g[:, spans[last]], whp[...])
    for k in range(last - 1, -1, -1):
        loads[k].wait()
        tk = t[spans[k], :]
        xk = (r * (1.0 - tk * tk)).astype(BF16)
        x[spans[k], :] = xk
        if k == last - 1:
            whole.wait()
        if k > 0:
            r = r + (dot_nt(xk, wh[...]) + dot_tn(g[:, spans[k]], whp[...]))
    inner = last * rows
    e[A_ROW : A_ROW + count, :] = dot(oh[...], x[...])[0:count, :]
    hid = sT.shape[0]
    half = hid // 2
    core, flip = place[0], place[1]
    for out, h in ((other, 1 - core), (mine, core)):
        left = sT[pl.ds(pl.multiple_of(h * half, half), half), :inner]
        for j in range(0, hid, 256):
            block = dot(left, x[:, j : j + 256])
            for p in range(2):
                slot = pl.ds((flip + p - 2 * flip * p) * 16, 16)
                for c in range(2):
                    n = j // LANES + c
                    out[slot, n * 16 : (n + 1) * 16, :] = block[
                        p * 256 : (p + 1) * 256, c * LANES : (c + 1) * LANES
                    ].reshape(16, 16, LANES)
        for i in range(4):
            p = i // 2
            slot = (flip + p - 2 * flip * p) * 16 + (i % 2) * 8
            rows8 = e[pl.ds(pl.multiple_of(h * 32 + i * 8, 8), 8), :]
            for n in range(8):
                out[slot + n, 128:136, :] = rows8[:, n * LANES : (n + 1) * LANES]


def plane_sum_kernel(arrived, out):
    total = arrived[0]
    for i in range(1, arrived.shape[0]):
        total = total + arrived[i]
    out[...] = total


def line_sum_kernel(own, near, far, both, out):
    total = (own[...] + near[...]) + (far[...] + both[...])
    for i in range(out.shape[0]):
        out[i] = total


def lay_out(place, part, h, gh_far, buf, e, sem):
    half = gh_far.shape[0] // 2
    flip = place[1]
    copies = []
    for p in range(2):
        slot = pl.ds((flip + p - 2 * flip * p) * 16, 16)
        here = slice(p * 256, (p + 1) * 256)
        for n in range(8):
            buf[here, n * LANES : (n + 1) * LANES] = part[
                slot, n * 16 : (n + 1) * 16, :
            ].reshape(256, LANES)
        at = pl.ds(pl.multiple_of(h * half + p * 256, 256), 256)
        copies.append(started(buf.at[here, :], gh_far.at[at, :], sem.at[p]))
    for i in range(4):
        p = i // 2
        slot = (flip + p - 2 * flip * p) * 16 + (i % 2) * 8
        at8 = pl.ds(pl.multiple_of(h * 32 + i * 8, 8), 8)
        for n in range(8):
            e[at8, n * LANES : (n + 1) * LANES] = part[slot + n, 128:136, :]
    return copies


def first_half_kernel(place, mine, gh_far, e, buf, sem):
    for copy in lay_out(place, mine, place[0], gh_far, buf, e, sem):
        copy.wait()


def second_half_kernel(place, other, e_in, gh_in, gh_far, ga, gd, buf, e, sem):
    e[...] = e_in[...]
    copies = lay_out(place, other, 1 - place[0], gh_far, buf, e, sem)
    ga[...] = e[A_ROW : A_ROW + ga.shape[0], :]
    gd[...] = e[0 : gd.shape[0], :]
    for copy in copies:
        copy.wait()


def shifted(array, axis, by):
    size = lax.axis_size(axis)
    return lax.ppermute(array, axis, [(i, (i + by) % size) for i in range(size)])


def of_group(part):
    return [part] + [shifted(part, "y", by) for by in (2, 1, 3)]


def swapped(tiles, axis):
    return lax.all_to_all(tiles, axis, split_axis=0, concat_axis=0, tiled=True)


def along_z(array, to):
    return lax.ppermute(array, LINE, [(z, to(z)) for z in range(8)])


def beside(z):
    return (z + 1 if z % 2 else z - 1) % 8


def across(z):
    return (z + 4) % 8


def body(embed, actions, rewards, ends, behaviour, w_hidden, w_action, w_heads):
    rows, hid = embed.shape
    steps = actions.shape[1]
    count = w_action.shape[0]
    groups = lax.axis_size("y")
    devices = lax.axis_size(ALL)
    place = jnp.stack([lax.axis_index("core"), lax.axis_index("zh") % 2]).astype(jnp.int32)

    s, t, out, ssq, act, whp = kernel_call(
        unroll_kernel,
        [
            ((steps * rows, hid), BF16),
            (((steps - 1) * rows, hid), F32),
            ((48, (steps + 1) * rows), F32),
            ((8, LANES), F32),
            ((steps, rows), jnp.int32),
            ((48, hid), BF16),
        ],
        (embed, actions.T, w_hidden, w_action, w_heads.T),
        (
            pltpu.VMEM((rows, hid), BF16),
            pltpu.VMEM((hid, hid), BF16),
            pltpu.VMEM((count, hid), BF16),
            pltpu.VMEM((2 * count, hid), BF16),
            pltpu.VMEM(((steps - 1) * rows, hid), F32),
            pltpu.VMEM((32, hid), BF16),
            pltpu.VMEM((48, hid), F32),
            pltpu.VMEM((40, hid), F32),
            pltpu.SemaphoreType.DMA((5,)),
            pltpu.SemaphoreType.DMA((steps - 1,)),
        ),
        far=range(5),
        far_outs=(1,),
    )
    ssqs = of_group(ssq)
    targets, tg, sT = kernel_call(
        targets_kernel,
        [((steps, rows), F32), ((steps, rows), F32), ((hid, steps * rows), BF16)],
        (rewards.T, ends.T, jnp.transpose(behaviour, (1, 2, 0)), act, s, out),
        (
            pltpu.VMEM((steps, rows), F32),
            pltpu.VMEM((steps, rows), jnp.int32),
            pltpu.VMEM((steps, count, rows), F32),
            pltpu.SemaphoreType.DMA((4,)),
        ),
        far=range(3),
        far_outs=(0,),
    )

    def weights_body(*refs):
        weights_kernel(groups, devices, count, *refs)

    a, b, mass = kernel_call(
        weights_body,
        [((48, steps * rows), F32), ((Q_ROW, steps * rows), F32), ((8, LANES), F32)],
        (act, out, tg, *ssqs),
    )
    masses = of_group(mass)

    def gradient_body(*refs):
        gradient_kernel(groups, count, *refs)

    parts = ((32, 136, LANES), F32)
    mine, other = kernel_call(
        gradient_body,
        [parts, parts],
        (place, act, a, b, *masses, sT, t, w_hidden, whp),
        (
            pltpu.VMEM((48, steps * rows), F32),
            pltpu.VMEM((48, steps * rows), BF16),
            pltpu.VMEM(((steps - 1) * rows, hid), BF16),
            pltpu.VMEM((32, (steps - 1) * rows), BF16),
            pltpu.VMEM((64, hid), F32),
            pltpu.VMEM(((steps - 1) * rows, hid), F32),
            pltpu.VMEM((hid, hid), BF16),
            pltpu.SemaphoreType.DMA((steps,)),
        ),
        scalars=1,
        far=(9, 10),
    )
    chip = mine + shifted(other, "core", 1)
    (own,) = kernel_call(plane_sum_kernel, [((136, LANES), F32)], (swapped(chip, NEAR),))
    far = along_z(own, across)
    both = along_z(own, lambda z: across(beside(z)))
    near = along_z(own, beside)
    (whole,) = kernel_call(line_sum_kernel, [parts], (own, near, far, both))
    mine = swapped(whole, NEAR)
    other = shifted(mine, "core", 1)
    staging = (pltpu.VMEM((hid // 2, hid), F32), pltpu.SemaphoreType.DMA((2,)))
    partly, extra = kernel_call(
        first_half_kernel,
        [((hid, hid), F32), ((64, hid), F32)],
        (place, mine),
        staging,
        scalars=1,
        far_outs=(0,),
    )
    grad_hidden, grad_action, grad_heads = kernel_call(
        second_half_kernel,
        [((hid, hid), F32), (w_action.shape, F32), (w_heads.shape[::-1], F32)],
        (place, other, extra, partly),
        (staging[0], pltpu.VMEM((64, hid), F32), staging[1]),
        scalars=1,
        far=(3,),
        far_outs=(0,),
        aliases={3: 0},
    )
    return (grad_hidden, grad_action, grad_heads.T, targets.T)


def solution(mesh):
    torus = Mesh(mesh.devices.reshape(4, 2, 4, 2, mesh.shape["batch"]), ALL)
    return jax.shard_map(
        body,
        mesh=torus,
        in_specs=(
            P(ALL, None),
            P(ALL, None),
            P(ALL, None),
            P(ALL, None),
            P(ALL, None, None),
            P(),
            P(),
            P(),
        ),
        out_specs=(P(), P(), P(), P(ALL, None)),
        check_vma=False,
    )
```

```python
import jax
import jax.numpy as jnp
from jax import lax
from jax.experimental import pallas as pl
from jax.experimental.pallas import tpu as pltpu
from jax.sharding import Mesh
from jax.sharding import PartitionSpec as P

ALL = ("zh", "zp", "x", "core", "y")
NEAR = ("zp", "x", "y")
LINE = ("zh", "zp")

DISCOUNT = 0.997
TRACE_LAMBDA = 0.95
EPSILON = 1e-06

LANES = 128
Q_ROW = 24
A_ROW = 40
F32 = jnp.float32
BF16 = jnp.bfloat16

VMEM = pl.BlockSpec(memory_space=pltpu.VMEM)
SMEM = pl.BlockSpec(memory_space=pltpu.SMEM)
FAR = pltpu.MemorySpace.HBM
HBM = pl.BlockSpec(memory_space=FAR)


def dot(a, b):
    return jnp.dot(a, b, preferred_element_type=F32)


def dot_nt(a, b):
    return lax.dot_general(a, b, (((1,), (1,)), ((), ())), preferred_element_type=F32)


def dot_tn(a, b):
    return lax.dot_general(a, b, (((0,), (0,)), ((), ())), preferred_element_type=F32)


def kernel_call(body, outs, inputs, scratch=(), scalars=0, far=(), far_outs=(), aliases=None):
    return pl.pallas_call(
        body,
        out_shape=tuple(
            FAR(s, d) if i in far_outs else jax.ShapeDtypeStruct(s, d)
            for i, (s, d) in enumerate(outs)
        ),
        in_specs=[
            SMEM if i < scalars else HBM if i in far else VMEM for i in range(len(inputs))
        ],
        out_specs=tuple(HBM if i in far_outs else VMEM for i in range(len(outs))),
        scratch_shapes=list(scratch),
        input_output_aliases=aliases or {},
        name=body.__name__,
        compiler_params=pltpu.CompilerParams(vmem_limit_bytes=16 * 1024 * 1024),
    )(*(pltpu.with_memory_space_constraint(x, FAR) if i in far else x for i, x in enumerate(inputs)))


def started(source, target, sem):
    copy = pltpu.make_async_copy(source, target, sem)
    copy.start()
    return copy


def chosen(act, step, count):
    columns = act.shape[1]
    return lax.broadcasted_iota(jnp.int32, (count, columns), 0) == act[step : step + 1, :]


def onehot_of(act, step):
    return chosen(act, step, 32).astype(F32).astype(BF16)


def policy_of(out, at, count):
    logits = out[0:count, at]
    q = out[Q_ROW : Q_ROW + count, at]
    e = jnp.exp(logits)
    total = jnp.sum(e, axis=0, keepdims=True)
    pi = e / total
    v = jnp.sum(pi * q, axis=0, keepdims=True)
    return logits, q, pi, total, v


def unroll_kernel(
    emb_far, act_far, wh_far, wa_far, whd_far,
    s_out, t_far, o_out, ssq_out, act, whp,
    emb, wh, wa, whd, t_buf, wap, wide, rows40, sem, t_sem,
):
    loads = [
        started(source, target, sem.at[i])
        for i, (source, target) in enumerate(
            ((wh_far, wh), (emb_far, emb), (act_far, act), (wa_far, wa), (whd_far, whd))
        )
    ]
    count = wa.shape[0]
    steps = act.shape[0]
    rows = emb.shape[0]
    wap[...] = jnp.zeros_like(wap)
    wide[...] = jnp.zeros_like(wide)
    for load in loads[1:]:
        load.wait()
    wap[:count, :] = wa[...]
    rows40[0 : 2 * count, :] = whd[...].astype(F32)
    wide[0:count, :] = rows40[0:count, :]
    wide[Q_ROW : Q_ROW + count, :] = rows40[count : 2 * count, :]
    whp[...] = wide[...].astype(BF16)
    state = emb[...].astype(F32)
    loads[0].wait()
    stores = []
    for k in range(steps):
        here = slice(k * rows, (k + 1) * rows)
        s = state.astype(BF16)
        s_out[here, :] = s
        t = jnp.tanh(dot(s, wh[...]) + dot_tn(onehot_of(act, k), wap[...]))
        if k < steps - 1:
            t_buf[here, :] = t
            stores.append(started(t_buf.at[here, :], t_far.at[here, :], t_sem.at[k]))
        state = state + t
    inner = steps * rows
    o_out[:, :inner] = dot_nt(whp[...], s_out[...])
    o_out[:, inner:] = dot_nt(whp[...], state.astype(BF16))
    _, q, _, _, v = policy_of(o_out, slice(0, inner), count)
    adv = q - v
    part = jnp.sum(jnp.sum(adv * adv, axis=1, keepdims=True), axis=0, keepdims=True)
    ssq_out[...] = jnp.broadcast_to(part, ssq_out.shape)
    for store in stores:
        store.wait()


def targets_kernel(rew_far, ends_far, beh_far, act, s, o, tg_far, tg_out, sT_out, rew, ends, beh, sem):
    loads = [
        started(source, target, sem.at[i])
        for i, (source, target) in enumerate(((rew_far, rew), (ends_far, ends), (beh_far, beh)))
    ]
    steps, rows = act.shape
    count = beh.shape[1]
    for k in range(steps):
        sT_out[:, k * rows : (k + 1) * rows] = s[k * rows : (k + 1) * rows, :].T
    for load in loads:
        load.wait()
    v_next = policy_of(o, slice(steps * rows, (steps + 1) * rows), count)[-1]
    carried = jnp.zeros((1, rows), F32)
    for k in range(steps - 1, -1, -1):
        logits, _, _, total, v = policy_of(o, slice(k * rows, (k + 1) * rows), count)
        b = beh[k]
        b_total = jnp.sum(jnp.exp(b), axis=0, keepdims=True)
        gap = (logits - jnp.log(total)) - (b - jnp.log(b_total))
        ratio = jnp.exp(jnp.sum(jnp.where(chosen(act, k, count), gap, 0.0), axis=0, keepdims=True))
        clipped = jnp.minimum(1.0, ratio)
        open_ = 1.0 - ends[k : k + 1, :].astype(F32)
        td = rew[k : k + 1, :] + DISCOUNT * open_ * v_next - v
        carried = clipped * td + DISCOUNT * TRACE_LAMBDA * open_ * clipped * carried
        tg_out[k : k + 1, :] = v + carried
        v_next = v
    started(tg_out, tg_far, sem.at[3]).wait()


def weights_kernel(groups, devices, count, act, o, tg, ssq0, ssq1, ssq2, ssq3, a_out, b_out, mass_out):
    steps, rows = act.shape
    spread = ssq0[0:1, 0:1] + ssq1[0:1, 0:1] + ssq2[0:1, 0:1] + ssq3[0:1, 0:1]
    scale = jnp.sqrt(spread / (groups * rows * steps * count) + EPSILON)
    norm = 1.0 / (devices * rows * steps)
    mass_sum = jnp.zeros((1, rows), F32)
    a_out[...] = jnp.zeros_like(a_out)
    b_out[...] = jnp.zeros_like(b_out)
    for k in range(steps):
        at = slice(k * rows, (k + 1) * rows)
        _, q, pi, _, v = policy_of(o, at, count)
        oh = chosen(act, k, count)
        w = jnp.exp(jnp.clip((q - v) / scale, -1.0, 1.0))
        pw = pi * w
        mass = jnp.sum(pw, axis=0, keepdims=True)
        mass_sum = mass_sum + mass
        cmpo = pw / mass
        whole = jnp.sum(cmpo, axis=0, keepdims=True)
        taken = jnp.sum(jnp.where(oh, w, 0.0), axis=0, keepdims=True)
        a_out[0:count, at] = (pi * whole - cmpo) * norm
        a_out[Q_ROW : Q_ROW + count, at] = jnp.where(oh, q - tg[k : k + 1, :], 0.0) * norm
        b_out[0:count, at] = taken * (pi - jnp.where(oh, 1.0, 0.0)) * norm
    mass_out[...] = jnp.broadcast_to(jnp.sum(mass_sum, axis=1, keepdims=True), mass_out.shape)


def gradient_kernel(
    groups, count, place, act, a, b, m0, m1, m2, m3, sT, t_far, wh_far, whp,
    mine, other, gf, g, x, oh, e, t, wh, sem,
):
    steps, rows = act.shape
    last = steps - 1
    spans = [slice(k * rows, (k + 1) * rows) for k in range(steps)]
    loads = {}
    for k in range(last - 1, -1, -1):
        loads[k] = started(t_far.at[spans[k], :], t.at[spans[k], :], sem.at[k])
        if k == last - 1:
            whole = started(wh_far, wh, sem.at[last])
    total = m0[0:1, 0:1] + m1[0:1, 0:1] + m2[0:1, 0:1] + m3[0:1, 0:1]
    mean = total / (groups * rows * steps)
    gf[...] = a[...]
    gf[0:Q_ROW, :] = a[0:Q_ROW, :] + b[...] / mean
    g[...] = gf[...].astype(BF16)
    for k in range(last):
        oh[:, spans[k]] = onehot_of(act, k)
    e[...] = jnp.zeros_like(e)
    heads = dot_nt(g[...], sT[...])
    e[0:count, :] = heads[0:count, :]
    e[count : 2 * count, :] = heads[Q_ROW : Q_ROW + count, :]
    r = dot_tn(g[:, spans[last]], whp[...])
    for k in range(last - 1, -1, -1):
        loads[k].wait()
        tk = t[spans[k], :]
        xk = (r * (1.0 - tk * tk)).astype(BF16)
        x[spans[k], :] = xk
        if k == last - 1:
            whole.wait()
        if k > 0:
            r = r + (dot_nt(xk, wh[...]) + dot_tn(g[:, spans[k]], whp[...]))
    inner = last * rows
    e[A_ROW : A_ROW + count, :] = dot(oh[...], x[...])[0:count, :]
    hid = sT.shape[0]
    half = hid // 2
    core, flip = place[0], place[1]
    for out, h in ((other, 1 - core), (mine, core)):
        left = sT[pl.ds(pl.multiple_of(h * half, half), half), :inner]
        for j in range(0, hid, 256):
            block = dot(left, x[:, j : j + 256])
            for p in range(2):
                slot = pl.ds((flip + p - 2 * flip * p) * 16, 16)
                for c in range(2):
                    n = j // LANES + c
                    out[slot, n * 16 : (n + 1) * 16, :] = block[
                        p * 256 : (p + 1) * 256, c * LANES : (c + 1) * LANES
                    ].reshape(16, 16, LANES)
        for i in range(4):
            p = i // 2
            slot = (flip + p - 2 * flip * p) * 16 + (i % 2) * 8
            rows8 = e[pl.ds(pl.multiple_of(h * 32 + i * 8, 8), 8), :]
            for n in range(8):
                out[slot + n, 128:136, :] = rows8[:, n * LANES : (n + 1) * LANES]


def plane_sum_kernel(arrived, out):
    total = arrived[0]
    for i in range(1, arrived.shape[0]):
        total = total + arrived[i]
    out[...] = total


def line_sum_kernel(own, near, far, both, out):
    total = (own[...] + near[...]) + (far[...] + both[...])
    for i in range(out.shape[0]):
        out[i] = total


def lay_out(place, part, h, gh_far, buf, e, sem):
    half = gh_far.shape[0] // 2
    flip = place[1]
    copies = []
    for p in range(2):
        slot = pl.ds((flip + p - 2 * flip * p) * 16, 16)
        here = slice(p * 256, (p + 1) * 256)
        for n in range(8):
            buf[here, n * LANES : (n + 1) * LANES] = part[
                slot, n * 16 : (n + 1) * 16, :
            ].reshape(256, LANES)
        at = pl.ds(pl.multiple_of(h * half + p * 256, 256), 256)
        copies.append(started(buf.at[here, :], gh_far.at[at, :], sem.at[p]))
    for i in range(4):
        p = i // 2
        slot = (flip + p - 2 * flip * p) * 16 + (i % 2) * 8
        at8 = pl.ds(pl.multiple_of(h * 32 + i * 8, 8), 8)
        for n in range(8):
            e[at8, n * LANES : (n + 1) * LANES] = part[slot + n, 128:136, :]
    return copies


def first_half_kernel(place, mine, gh_far, e, buf, sem):
    for copy in lay_out(place, mine, place[0], gh_far, buf, e, sem):
        copy.wait()


def second_half_kernel(place, other, e_in, gh_in, gh_far, ga, gd, buf, e, sem):
    e[...] = e_in[...]
    copies = lay_out(place, other, 1 - place[0], gh_far, buf, e, sem)
    ga[...] = e[A_ROW : A_ROW + ga.shape[0], :]
    gd[...] = e[0 : gd.shape[0], :]
    for copy in copies:
        copy.wait()


def shifted(array, axis, by):
    size = lax.axis_size(axis)
    return lax.ppermute(array, axis, [(i, (i + by) % size) for i in range(size)])


def of_group(part):
    return [part] + [shifted(part, "y", by) for by in (2, 1, 3)]


def swapped(tiles, axis):
    return lax.all_to_all(tiles, axis, split_axis=0, concat_axis=0, tiled=True)


def along_z(array, to):
    return lax.ppermute(array, LINE, [(z, to(z)) for z in range(8)])


def beside(z):
    return (z + 1 if z % 2 else z - 1) % 8


def across(z):
    return (z + 4) % 8


def body(embed, actions, rewards, ends, behaviour, w_hidden, w_action, w_heads):
    rows, hid = embed.shape
    steps = actions.shape[1]
    count = w_action.shape[0]
    groups = lax.axis_size("y")
    devices = lax.axis_size(ALL)
    place = jnp.stack([lax.axis_index("core"), lax.axis_index("zh") % 2]).astype(jnp.int32)

    s, t, out, ssq, act, whp = kernel_call(
        unroll_kernel,
        [
            ((steps * rows, hid), BF16),
            (((steps - 1) * rows, hid), F32),
            ((48, (steps + 1) * rows), F32),
            ((8, LANES), F32),
            ((steps, rows), jnp.int32),
            ((48, hid), BF16),
        ],
        (embed, actions.T, w_hidden, w_action, w_heads.T),
        (
            pltpu.VMEM((rows, hid), BF16),
            pltpu.VMEM((hid, hid), BF16),
            pltpu.VMEM((count, hid), BF16),
            pltpu.VMEM((2 * count, hid), BF16),
            pltpu.VMEM(((steps - 1) * rows, hid), F32),
            pltpu.VMEM((32, hid), BF16),
            pltpu.VMEM((48, hid), F32),
            pltpu.VMEM((40, hid), F32),
            pltpu.SemaphoreType.DMA((5,)),
            pltpu.SemaphoreType.DMA((steps - 1,)),
        ),
        far=range(5),
        far_outs=(1,),
    )
    ssqs = of_group(ssq)
    targets, tg, sT = kernel_call(
        targets_kernel,
        [((steps, rows), F32), ((steps, rows), F32), ((hid, steps * rows), BF16)],
        (rewards.T, ends.T, jnp.transpose(behaviour, (1, 2, 0)), act, s, out),
        (
            pltpu.VMEM((steps, rows), F32),
            pltpu.VMEM((steps, rows), jnp.int32),
            pltpu.VMEM((steps, count, rows), F32),
            pltpu.SemaphoreType.DMA((4,)),
        ),
        far=range(3),
        far_outs=(0,),
    )

    def weights_body(*refs):
        weights_kernel(groups, devices, count, *refs)

    a, b, mass = kernel_call(
        weights_body,
        [((48, steps * rows), F32), ((Q_ROW, steps * rows), F32), ((8, LANES), F32)],
        (act, out, tg, *ssqs),
    )
    masses = of_group(mass)

    def gradient_body(*refs):
        gradient_kernel(groups, count, *refs)

    parts = ((32, 136, LANES), F32)
    mine, other = kernel_call(
        gradient_body,
        [parts, parts],
        (place, act, a, b, *masses, sT, t, w_hidden, whp),
        (
            pltpu.VMEM((48, steps * rows), F32),
            pltpu.VMEM((48, steps * rows), BF16),
            pltpu.VMEM(((steps - 1) * rows, hid), BF16),
            pltpu.VMEM((32, (steps - 1) * rows), BF16),
            pltpu.VMEM((64, hid), F32),
            pltpu.VMEM(((steps - 1) * rows, hid), F32),
            pltpu.VMEM((hid, hid), BF16),
            pltpu.SemaphoreType.DMA((steps,)),
        ),
        scalars=1,
        far=(9, 10),
    )
    chip = mine + shifted(other, "core", 1)
    (own,) = kernel_call(plane_sum_kernel, [((136, LANES), F32)], (swapped(chip, NEAR),))
    far = along_z(own, across)
    both = along_z(own, lambda z: across(beside(z)))
    near = along_z(own, beside)
    (whole,) = kernel_call(line_sum_kernel, [parts], (own, near, far, both))
    mine = swapped(whole, NEAR)
    other = shifted(mine, "core", 1)
    staging = (pltpu.VMEM((hid // 2, hid), F32), pltpu.SemaphoreType.DMA((2,)))
    partly, extra = kernel_call(
        first_half_kernel,
        [((hid, hid), F32), ((64, hid), F32)],
        (place, mine),
        staging,
        scalars=1,
        far_outs=(0,),
    )
    grad_hidden, grad_action, grad_heads = kernel_call(
        second_half_kernel,
        [((hid, hid), F32), (w_action.shape, F32), (w_heads.shape[::-1], F32)],
        (place, other, extra, partly),
        (staging[0], pltpu.VMEM((64, hid), F32), staging[1]),
        scalars=1,
        far=(3,),
        far_outs=(0,),
        aliases={3: 0},
    )
    return (grad_hidden, grad_action, grad_heads.T, targets.T)


def solution(mesh):
    torus = Mesh(mesh.devices.reshape(4, 2, 4, 2, mesh.shape["batch"]), ALL)
    return jax.shard_map(
        body,
        mesh=torus,
        in_specs=(
            P(ALL, None),
            P(ALL, None),
            P(ALL, None),
            P(ALL, None),
            P(ALL, None, None),
            P(),
            P(),
            P(),
        ),
        out_specs=(P(), P(), P(), P(ALL, None)),
        check_vma=False,
    )
```

```python
import jax
import jax.numpy as jnp
from jax import lax
from jax.experimental import pallas as pl
from jax.experimental.pallas import tpu as pltpu
from jax.sharding import Mesh
from jax.sharding import PartitionSpec as P

ALL = ("zh", "zp", "x", "core", "y")
NEAR = ("zp", "x", "y")
LINE = ("zh", "zp")

DISCOUNT = 0.997
TRACE_LAMBDA = 0.95
EPSILON = 1e-06

LANES = 128
Q_ROW = 24
A_ROW = 40
F32 = jnp.float32
BF16 = jnp.bfloat16

VMEM = pl.BlockSpec(memory_space=pltpu.VMEM)
SMEM = pl.BlockSpec(memory_space=pltpu.SMEM)
FAR = pltpu.MemorySpace.HBM
HBM = pl.BlockSpec(memory_space=FAR)


def dot(a, b):
    return jnp.dot(a, b, preferred_element_type=F32)


def dot_nt(a, b):
    return lax.dot_general(a, b, (((1,), (1,)), ((), ())), preferred_element_type=F32)


def dot_tn(a, b):
    return lax.dot_general(a, b, (((0,), (0,)), ((), ())), preferred_element_type=F32)


def kernel_call(body, outs, inputs, scratch=(), scalars=0, far=(), far_outs=(), aliases=None):
    return pl.pallas_call(
        body,
        out_shape=tuple(
            FAR(s, d) if i in far_outs else jax.ShapeDtypeStruct(s, d)
            for i, (s, d) in enumerate(outs)
        ),
        in_specs=[
            SMEM if i < scalars else HBM if i in far else VMEM for i in range(len(inputs))
        ],
        out_specs=tuple(HBM if i in far_outs else VMEM for i in range(len(outs))),
        scratch_shapes=list(scratch),
        input_output_aliases=aliases or {},
        name=body.__name__,
        compiler_params=pltpu.CompilerParams(vmem_limit_bytes=16 * 1024 * 1024),
    )(*(pltpu.with_memory_space_constraint(x, FAR) if i in far else x for i, x in enumerate(inputs)))


def started(source, target, sem):
    copy = pltpu.make_async_copy(source, target, sem)
    copy.start()
    return copy


def chosen(act, step, count):
    columns = act.shape[1]
    return lax.broadcasted_iota(jnp.int32, (count, columns), 0) == act[step : step + 1, :]


def onehot_of(act, step):
    return chosen(act, step, 32).astype(F32).astype(BF16)


def policy_of(out, at, count):
    logits = out[0:count, at]
    q = out[Q_ROW : Q_ROW + count, at]
    e = jnp.exp(logits)
    total = jnp.sum(e, axis=0, keepdims=True)
    pi = e / total
    v = jnp.sum(pi * q, axis=0, keepdims=True)
    return logits, q, pi, total, v


def unroll_kernel(
    emb_far, act_far, wh_far, wa_far, whd_far,
    s_out, t_far, o_out, ssq_out, act, whp,
    emb, wh, wa, whd, t_buf, wap, wide, rows40, sem, t_sem,
):
    loads = [
        started(source, target, sem.at[i])
        for i, (source, target) in enumerate(
            ((wh_far, wh), (emb_far, emb), (act_far, act), (wa_far, wa), (whd_far, whd))
        )
    ]
    count = wa.shape[0]
    steps = act.shape[0]
    rows = emb.shape[0]
    wap[...] = jnp.zeros_like(wap)
    wide[...] = jnp.zeros_like(wide)
    for load in loads[1:]:
        load.wait()
    wap[:count, :] = wa[...]
    rows40[0 : 2 * count, :] = whd[...].astype(F32)
    wide[0:count, :] = rows40[0:count, :]
    wide[Q_ROW : Q_ROW + count, :] = rows40[count : 2 * count, :]
    whp[...] = wide[...].astype(BF16)
    state = emb[...].astype(F32)
    loads[0].wait()
    stores = []
    for k in range(steps):
        here = slice(k * rows, (k + 1) * rows)
        s = state.astype(BF16)
        s_out[here, :] = s
        t = jnp.tanh(dot(s, wh[...]) + dot_tn(onehot_of(act, k), wap[...]))
        if k < steps - 1:
            t_buf[here, :] = t
            stores.append(started(t_buf.at[here, :], t_far.at[here, :], t_sem.at[k]))
        state = state + t
    inner = steps * rows
    o_out[:, :inner] = dot_nt(whp[...], s_out[...])
    o_out[:, inner:] = dot_nt(whp[...], state.astype(BF16))
    _, q, _, _, v = policy_of(o_out, slice(0, inner), count)
    adv = q - v
    part = jnp.sum(jnp.sum(adv * adv, axis=1, keepdims=True), axis=0, keepdims=True)
    ssq_out[...] = jnp.broadcast_to(part, ssq_out.shape)
    for store in stores:
        store.wait()


def targets_kernel(rew_far, ends_far, beh_far, act, s, o, tg_far, tg_out, sT_out, rew, ends, beh, sem):
    loads = [
        started(source, target, sem.at[i])
        for i, (source, target) in enumerate(((rew_far, rew), (ends_far, ends), (beh_far, beh)))
    ]
    steps, rows = act.shape
    count = beh.shape[1]
    for k in range(steps):
        sT_out[:, k * rows : (k + 1) * rows] = s[k * rows : (k + 1) * rows, :].T
    for load in loads:
        load.wait()
    v_next = policy_of(o, slice(steps * rows, (steps + 1) * rows), count)[-1]
    carried = jnp.zeros((1, rows), F32)
    for k in range(steps - 1, -1, -1):
        logits, _, _, total, v = policy_of(o, slice(k * rows, (k + 1) * rows), count)
        b = beh[k]
        b_total = jnp.sum(jnp.exp(b), axis=0, keepdims=True)
        gap = (logits - jnp.log(total)) - (b - jnp.log(b_total))
        ratio = jnp.exp(jnp.sum(jnp.where(chosen(act, k, count), gap, 0.0), axis=0, keepdims=True))
        clipped = jnp.minimum(1.0, ratio)
        open_ = 1.0 - ends[k : k + 1, :].astype(F32)
        td = rew[k : k + 1, :] + DISCOUNT * open_ * v_next - v
        carried = clipped * td + DISCOUNT * TRACE_LAMBDA * open_ * clipped * carried
        tg_out[k : k + 1, :] = v + carried
        v_next = v
    started(tg_out, tg_far, sem.at[3]).wait()


def weights_kernel(groups, devices, count, act, o, tg, ssq0, ssq1, ssq2, ssq3, a_out, b_out, mass_out):
    steps, rows = act.shape
    spread = ssq0[0:1, 0:1] + ssq1[0:1, 0:1] + ssq2[0:1, 0:1] + ssq3[0:1, 0:1]
    scale = jnp.sqrt(spread / (groups * rows * steps * count) + EPSILON)
    norm = 1.0 / (devices * rows * steps)
    mass_sum = jnp.zeros((1, rows), F32)
    a_out[...] = jnp.zeros_like(a_out)
    b_out[...] = jnp.zeros_like(b_out)
    for k in range(steps):
        at = slice(k * rows, (k + 1) * rows)
        _, q, pi, _, v = policy_of(o, at, count)
        oh = chosen(act, k, count)
        w = jnp.exp(jnp.clip((q - v) / scale, -1.0, 1.0))
        pw = pi * w
        mass = jnp.sum(pw, axis=0, keepdims=True)
        mass_sum = mass_sum + mass
        cmpo = pw / mass
        whole = jnp.sum(cmpo, axis=0, keepdims=True)
        taken = jnp.sum(jnp.where(oh, w, 0.0), axis=0, keepdims=True)
        a_out[0:count, at] = (pi * whole - cmpo) * norm
        a_out[Q_ROW : Q_ROW + count, at] = jnp.where(oh, q - tg[k : k + 1, :], 0.0) * norm
        b_out[0:count, at] = taken * (pi - jnp.where(oh, 1.0, 0.0)) * norm
    mass_out[...] = jnp.broadcast_to(jnp.sum(mass_sum, axis=1, keepdims=True), mass_out.shape)


def fetch_kernel(t_far, wh_far, after, t, wh, sem):
    for copy in (started(t_far, t, sem.at[0]), started(wh_far, wh, sem.at[1])):
        copy.wait()


def gradient_kernel(
    groups, count, place, act, a, b, m0, m1, m2, m3, sT, t, wh, whp,
    other, x, e, gf, g, oh,
):
    steps, rows = act.shape
    last = steps - 1
    spans = [slice(k * rows, (k + 1) * rows) for k in range(steps)]
    total = m0[0:1, 0:1] + m1[0:1, 0:1] + m2[0:1, 0:1] + m3[0:1, 0:1]
    mean = total / (groups * rows * steps)
    gf[...] = a[...]
    gf[0:Q_ROW, :] = a[0:Q_ROW, :] + b[...] / mean
    g[...] = gf[...].astype(BF16)
    for k in range(last):
        oh[:, spans[k]] = onehot_of(act, k)
    e[...] = jnp.zeros_like(e)
    heads = dot_nt(g[...], sT[...])
    e[0:count, :] = heads[0:count, :]
    e[count : 2 * count, :] = heads[Q_ROW : Q_ROW + count, :]
    r = dot_tn(g[:, spans[last]], whp[...])
    for k in range(last - 1, -1, -1):
        tk = t[spans[k], :]
        xk = (r * (1.0 - tk * tk)).astype(BF16)
        x[spans[k], :] = xk
        if k > 0:
            r = r + (dot_nt(xk, wh[...]) + dot_tn(g[:, spans[k]], whp[...]))
    inner = last * rows
    e[A_ROW : A_ROW + count, :] = dot(oh[...], x[...])[0:count, :]
    tile_half(place, 1 - place[0], sT, x, e, other)


def tile_half(place, h, sT, x, e, out):
    hid = sT.shape[0]
    half = hid // 2
    flip = place[1]
    left = sT[pl.ds(pl.multiple_of(h * half, half), half), : x.shape[0]]
    for j in range(0, hid, 256):
        block = dot(left, x[:, j : j + 256])
        for p in range(2):
            slot = pl.ds((flip + p - 2 * flip * p) * 16, 16)
            for c in range(2):
                n = j // LANES + c
                out[slot, n * 16 : (n + 1) * 16, :] = block[
                    p * 256 : (p + 1) * 256, c * LANES : (c + 1) * LANES
                ].reshape(16, 16, LANES)
    for i in range(4):
        p = i // 2
        slot = (flip + p - 2 * flip * p) * 16 + (i % 2) * 8
        rows8 = e[pl.ds(pl.multiple_of(h * 32 + i * 8, 8), 8), :]
        for n in range(8):
            out[slot + n, 128:136, :] = rows8[:, n * LANES : (n + 1) * LANES]


def mine_kernel(place, sT, x, e, out):
    tile_half(place, place[0], sT, x, e, out)


def plane_sum_kernel(arrived, out):
    total = arrived[0]
    for i in range(1, arrived.shape[0]):
        total = total + arrived[i]
    out[...] = total


def line_sum_kernel(own, near, far, both, out):
    total = (own[...] + near[...]) + (far[...] + both[...])
    for i in range(out.shape[0]):
        out[i] = total


def lay_out(place, part, h, gh_far, e, sem):
    units = part.shape[0]
    flip = place[1]
    copies = []
    for p in range(2):
        slot = pl.ds((flip + p - 2 * flip * p) * 16, 16)
        at = pl.ds(h * units + p * 16, 16)
        for n in range(8):
            copies.append(
                started(
                    part.at[slot, n * 16 : (n + 1) * 16, :],
                    gh_far.at[at, :, n * LANES : (n + 1) * LANES],
                    sem.at[p * 8 + n],
                )
            )
    for i in range(4):
        p = i // 2
        slot = (flip + p - 2 * flip * p) * 16 + (i % 2) * 8
        at8 = pl.ds(pl.multiple_of(h * 32 + i * 8, 8), 8)
        for n in range(8):
            e[at8, n * LANES : (n + 1) * LANES] = part[slot + n, 128:136, :]
    return copies


def first_half_kernel(place, mine, gh_far, e, sem):
    e[...] = jnp.zeros_like(e)
    for copy in lay_out(place, mine, place[0], gh_far, e, sem):
        copy.wait()


def second_half_kernel(place, other, e_in, gh_in, gh_far, ga_far, gd_far, e, ga, gd, sem):
    e[...] = e_in[...]
    copies = lay_out(place, other, 1 - place[0], gh_far, e, sem)
    ga[...] = e[A_ROW : A_ROW + ga.shape[0], :]
    copies.append(started(ga, ga_far, sem.at[16]))
    gd[...] = e[0 : gd.shape[0], :]
    copies.append(started(gd, gd_far, sem.at[17]))
    for copy in copies:
        copy.wait()


def shifted(array, axis, by):
    size = lax.axis_size(axis)
    return lax.ppermute(array, axis, [(i, (i + by) % size) for i in range(size)])


def of_group(part):
    return [part] + [shifted(part, "y", by) for by in (2, 1, 3)]


def swapped(tiles, axis):
    return lax.all_to_all(tiles, axis, split_axis=0, concat_axis=0, tiled=True)


def along_z(array, to):
    return lax.ppermute(array, LINE, [(z, to(z)) for z in range(8)])


def beside(z):
    return (z + 1 if z % 2 else z - 1) % 8


def across(z):
    return (z + 4) % 8


def body(embed, actions, rewards, ends, behaviour, w_hidden, w_action, w_heads):
    rows, hid = embed.shape
    steps = actions.shape[1]
    count = w_action.shape[0]
    groups = lax.axis_size("y")
    devices = lax.axis_size(ALL)
    place = jnp.stack([lax.axis_index("core"), lax.axis_index("zh") % 2]).astype(jnp.int32)

    s, t, out, ssq, act, whp = kernel_call(
        unroll_kernel,
        [
            ((steps * rows, hid), BF16),
            (((steps - 1) * rows, hid), F32),
            ((48, (steps + 1) * rows), F32),
            ((8, LANES), F32),
            ((steps, rows), jnp.int32),
            ((48, hid), BF16),
        ],
        (embed, actions.T, w_hidden, w_action, w_heads.T),
        (
            pltpu.VMEM((rows, hid), BF16),
            pltpu.VMEM((hid, hid), BF16),
            pltpu.VMEM((count, hid), BF16),
            pltpu.VMEM((2 * count, hid), BF16),
            pltpu.VMEM(((steps - 1) * rows, hid), F32),
            pltpu.VMEM((32, hid), BF16),
            pltpu.VMEM((48, hid), F32),
            pltpu.VMEM((40, hid), F32),
            pltpu.SemaphoreType.DMA((5,)),
            pltpu.SemaphoreType.DMA((steps - 1,)),
        ),
        far=range(5),
        far_outs=(1,),
    )
    ssqs = of_group(ssq)
    targets, tg, sT = kernel_call(
        targets_kernel,
        [((steps, rows), F32), ((steps, rows), F32), ((hid, steps * rows), BF16)],
        (rewards.T, ends.T, jnp.transpose(behaviour, (1, 2, 0)), act, s, out),
        (
            pltpu.VMEM((steps, rows), F32),
            pltpu.VMEM((steps, rows), jnp.int32),
            pltpu.VMEM((steps, count, rows), F32),
            pltpu.SemaphoreType.DMA((4,)),
        ),
        far=range(3),
        far_outs=(0,),
    )

    def weights_body(*refs):
        weights_kernel(groups, devices, count, *refs)

    a, b, mass = kernel_call(
        weights_body,
        [((48, steps * rows), F32), ((Q_ROW, steps * rows), F32), ((8, LANES), F32)],
        (act, out, tg, *ssqs),
    )
    masses = of_group(mass)

    t, wh = kernel_call(
        fetch_kernel,
        [(t.shape, F32), (w_hidden.shape, BF16)],
        (t, w_hidden, mass),
        (pltpu.SemaphoreType.DMA((2,)),),
        far=(0, 1),
    )

    def gradient_body(*refs):
        gradient_kernel(groups, count, *refs)

    parts = ((32, 136, LANES), F32)
    other, x, extra = kernel_call(
        gradient_body,
        [parts, (((steps - 1) * rows, hid), BF16), ((64, hid), F32)],
        (place, act, a, b, *masses, sT, t, wh, whp),
        (
            pltpu.VMEM((48, steps * rows), F32),
            pltpu.VMEM((48, steps * rows), BF16),
            pltpu.VMEM((32, (steps - 1) * rows), BF16),
        ),
        scalars=1,
    )
    arriving = shifted(other, "core", 1)
    (mine,) = kernel_call(mine_kernel, [parts], (place, sT, x, extra), scalars=1)
    chip = mine + arriving
    (own,) = kernel_call(plane_sum_kernel, [((136, LANES), F32)], (swapped(chip, NEAR),))
    far = along_z(own, across)
    both = along_z(own, lambda z: across(beside(z)))
    near = along_z(own, beside)
    (whole,) = kernel_call(line_sum_kernel, [parts], (own, near, far, both))
    mine = swapped(whole, NEAR)
    other = shifted(mine, "core", 1)
    copied = pltpu.SemaphoreType.DMA((16,))
    tiles = ((64, 16, hid), F32)
    partly, extra = kernel_call(
        first_half_kernel,
        [tiles, ((64, hid), F32)],
        (place, mine),
        (copied,),
        scalars=1,
        far_outs=(0,),
    )
    grad_hidden, grad_action, grad_heads = kernel_call(
        second_half_kernel,
        [tiles, (w_action.shape, F32), (w_heads.shape[::-1], F32)],
        (place, other, extra, partly),
        (
            pltpu.VMEM((64, hid), F32),
            pltpu.VMEM(w_action.shape, F32),
            pltpu.VMEM(w_heads.shape[::-1], F32),
            pltpu.SemaphoreType.DMA((18,)),
        ),
        scalars=1,
        far=(3,),
        far_outs=(0, 1, 2),
        aliases={3: 0},
    )
    return (grad_hidden.reshape(hid, hid), grad_action, grad_heads.T, targets.T)


def solution(mesh):
    torus = Mesh(mesh.devices.reshape(4, 2, 4, 2, mesh.shape["batch"]), ALL)
    return jax.shard_map(
        body,
        mesh=torus,
        in_specs=(
            P(ALL, None),
            P(ALL, None),
            P(ALL, None),
            P(ALL, None),
            P(ALL, None, None),
            P(),
            P(),
            P(),
        ),
        out_specs=(P(), P(), P(), P(ALL, None)),
        check_vma=False,
    )
```

```python
import jax
import jax.numpy as jnp
from jax import lax
from jax.experimental import pallas as pl
from jax.experimental.pallas import tpu as pltpu
from jax.sharding import Mesh
from jax.sharding import PartitionSpec as P

ALL = ("zh", "zp", "x", "core", "y")
NEAR = ("zp", "x", "y")
LINE = ("zh", "zp")

DISCOUNT = 0.997
TRACE_LAMBDA = 0.95
EPSILON = 1e-06

LANES = 128
Q_ROW = 24
A_ROW = 40
F32 = jnp.float32
BF16 = jnp.bfloat16

VMEM = pl.BlockSpec(memory_space=pltpu.VMEM)
SMEM = pl.BlockSpec(memory_space=pltpu.SMEM)
FAR = pltpu.MemorySpace.HBM
HBM = pl.BlockSpec(memory_space=FAR)


def dot(a, b):
    return jnp.dot(a, b, preferred_element_type=F32)


def dot_nt(a, b):
    return lax.dot_general(a, b, (((1,), (1,)), ((), ())), preferred_element_type=F32)


def dot_tn(a, b):
    return lax.dot_general(a, b, (((0,), (0,)), ((), ())), preferred_element_type=F32)


def kernel_call(body, outs, inputs, scratch=(), scalars=0, far=(), far_outs=(), aliases=None):
    return pl.pallas_call(
        body,
        out_shape=tuple(
            FAR(s, d) if i in far_outs else jax.ShapeDtypeStruct(s, d)
            for i, (s, d) in enumerate(outs)
        ),
        in_specs=[
            SMEM if i < scalars else HBM if i in far else VMEM for i in range(len(inputs))
        ],
        out_specs=tuple(HBM if i in far_outs else VMEM for i in range(len(outs))),
        scratch_shapes=list(scratch),
        input_output_aliases=aliases or {},
        name=body.__name__,
        compiler_params=pltpu.CompilerParams(vmem_limit_bytes=16 * 1024 * 1024),
    )(*(pltpu.with_memory_space_constraint(x, FAR) if i in far else x for i, x in enumerate(inputs)))


def started(source, target, sem):
    copy = pltpu.make_async_copy(source, target, sem)
    copy.start()
    return copy


def chosen(act, step, count):
    columns = act.shape[1]
    return lax.broadcasted_iota(jnp.int32, (count, columns), 0) == act[step : step + 1, :]


def onehot_of(act, step):
    return chosen(act, step, 32).astype(F32).astype(BF16)


def policy_of(out, at, count):
    logits = out[0:count, at]
    q = out[Q_ROW : Q_ROW + count, at]
    e = jnp.exp(logits)
    total = jnp.sum(e, axis=0, keepdims=True)
    pi = e / total
    v = jnp.sum(pi * q, axis=0, keepdims=True)
    return logits, q, pi, total, v


def unroll_kernel(
    emb_far, act_far, wh_far, wa_far, whd_far,
    s_out, t_far, o_out, ssq_out, act, whp,
    emb, wh, wa, whd, t_buf, wap, wide, rows40, sem, t_sem,
):
    loads = [
        started(source, target, sem.at[i])
        for i, (source, target) in enumerate(
            ((wh_far, wh), (emb_far, emb), (act_far, act), (wa_far, wa), (whd_far, whd))
        )
    ]
    count = wa.shape[0]
    steps = act.shape[0]
    rows = emb.shape[0]
    wap[...] = jnp.zeros_like(wap)
    wide[...] = jnp.zeros_like(wide)
    for load in loads[1:]:
        load.wait()
    wap[:count, :] = wa[...]
    rows40[0 : 2 * count, :] = whd[...].astype(F32)
    wide[0:count, :] = rows40[0:count, :]
    wide[Q_ROW : Q_ROW + count, :] = rows40[count : 2 * count, :]
    whp[...] = wide[...].astype(BF16)
    state = emb[...].astype(F32)
    loads[0].wait()
    stores = []
    for k in range(steps):
        here = slice(k * rows, (k + 1) * rows)
        s = state.astype(BF16)
        s_out[here, :] = s
        t = jnp.tanh(dot(s, wh[...]) + dot_tn(onehot_of(act, k), wap[...]))
        if k < steps - 1:
            t_buf[here, :] = t
            stores.append(started(t_buf.at[here, :], t_far.at[here, :], t_sem.at[k]))
        state = state + t
    inner = steps * rows
    o_out[:, :inner] = dot_nt(whp[...], s_out[...])
    o_out[:, inner:] = dot_nt(whp[...], state.astype(BF16))
    _, q, _, _, v = policy_of(o_out, slice(0, inner), count)
    adv = q - v
    part = jnp.sum(jnp.sum(adv * adv, axis=1, keepdims=True), axis=0, keepdims=True)
    ssq_out[...] = jnp.broadcast_to(part, ssq_out.shape)
    for store in stores:
        store.wait()


def targets_kernel(
    rew_far, ends_far, beh_far, act, s, o, tg_far, pi_out, adv_out, dq_out, sT_out,
    rew, ends, beh, tg_out, sem,
):
    loads = [
        started(source, target, sem.at[i])
        for i, (source, target) in enumerate(((rew_far, rew), (ends_far, ends), (beh_far, beh)))
    ]
    steps, rows = act.shape
    count = beh.shape[1]
    for k in range(steps):
        sT_out[:, k * rows : (k + 1) * rows] = s[k * rows : (k + 1) * rows, :].T
    for load in loads:
        load.wait()
    v_next = policy_of(o, slice(steps * rows, (steps + 1) * rows), count)[-1]
    carried = jnp.zeros((1, rows), F32)
    for k in range(steps - 1, -1, -1):
        at = slice(k * rows, (k + 1) * rows)
        logits, q, pi, total, v = policy_of(o, at, count)
        pi_out[:, at] = pi
        adv_out[:, at] = q - v
        b = beh[k]
        b_total = jnp.sum(jnp.exp(b), axis=0, keepdims=True)
        gap = (logits - jnp.log(total)) - (b - jnp.log(b_total))
        oh = chosen(act, k, count)
        ratio = jnp.exp(jnp.sum(jnp.where(oh, gap, 0.0), axis=0, keepdims=True))
        clipped = jnp.minimum(1.0, ratio)
        open_ = 1.0 - ends[k : k + 1, :].astype(F32)
        td = rew[k : k + 1, :] + DISCOUNT * open_ * v_next - v
        carried = clipped * td + DISCOUNT * TRACE_LAMBDA * open_ * clipped * carried
        tg_out[k : k + 1, :] = v + carried
        dq_out[:, at] = jnp.where(oh, q - (v + carried), 0.0)
        v_next = v
    started(tg_out, tg_far, sem.at[3]).wait()


def weights_kernel(groups, devices, act, pis, advs, dqs, ssq0, ssq1, ssq2, ssq3, a_out, b_out, mass_out):
    steps, rows = act.shape
    count = pis.shape[0]
    spread = ssq0[0:1, 0:1] + ssq1[0:1, 0:1] + ssq2[0:1, 0:1] + ssq3[0:1, 0:1]
    scale = jnp.sqrt(spread / (groups * rows * steps * count) + EPSILON)
    norm = 1.0 / (devices * rows * steps)
    mass_sum = jnp.zeros((1, rows), F32)
    a_out[...] = jnp.zeros_like(a_out)
    b_out[...] = jnp.zeros_like(b_out)
    for k in range(steps):
        at = slice(k * rows, (k + 1) * rows)
        pi = pis[:, at]
        oh = chosen(act, k, count)
        w = jnp.exp(jnp.clip(advs[:, at] / scale, -1.0, 1.0))
        pw = pi * w
        mass = jnp.sum(pw, axis=0, keepdims=True)
        mass_sum = mass_sum + mass
        cmpo = pw / mass
        whole = jnp.sum(cmpo, axis=0, keepdims=True)
        taken = jnp.sum(jnp.where(oh, w, 0.0), axis=0, keepdims=True)
        a_out[0:count, at] = (pi * whole - cmpo) * norm
        a_out[Q_ROW : Q_ROW + count, at] = dqs[:, at] * norm
        b_out[0:count, at] = taken * (pi - jnp.where(oh, 1.0, 0.0)) * norm
    mass_out[...] = jnp.broadcast_to(jnp.sum(mass_sum, axis=1, keepdims=True), mass_out.shape)


def fetch_kernel(t_far, wh_far, act, after, t, wh, oh, sem):
    copies = started(t_far, t, sem.at[0]), started(wh_far, wh, sem.at[1])
    steps, rows = act.shape
    for k in range(steps - 1):
        oh[:, k * rows : (k + 1) * rows] = onehot_of(act, k)
    for copy in copies:
        copy.wait()


def gradient_kernel(
    groups, count, place, act, a, b, m0, m1, m2, m3, s, sT, t, wh, whp, oh,
    other, x, e, gf, g,
):
    steps, rows = act.shape
    last = steps - 1
    spans = [slice(k * rows, (k + 1) * rows) for k in range(steps)]
    total = m0[0:1, 0:1] + m1[0:1, 0:1] + m2[0:1, 0:1] + m3[0:1, 0:1]
    mean = total / (groups * rows * steps)
    gf[...] = a[...]
    gf[0:Q_ROW, :] = a[0:Q_ROW, :] + b[...] / mean
    g[...] = gf[...].astype(BF16)
    e[...] = jnp.zeros_like(e)
    heads = dot(g[...], s[...])
    e[0:count, :] = heads[0:count, :]
    e[count : 2 * count, :] = heads[Q_ROW : Q_ROW + count, :]
    r = dot_tn(g[:, spans[last]], whp[...])
    for k in range(last - 1, -1, -1):
        tk = t[spans[k], :]
        xk = (r * (1.0 - tk * tk)).astype(BF16)
        x[spans[k], :] = xk
        if k > 0:
            r = r + (dot_nt(xk, wh[...]) + dot_tn(g[:, spans[k]], whp[...]))
    inner = last * rows
    e[A_ROW : A_ROW + count, :] = dot(oh[...], x[...])[0:count, :]
    tile_half(place, 1 - place[0], sT, x, e, other)


def tile_half(place, h, sT, x, e, out):
    hid = sT.shape[0]
    half = hid // 2
    flip = place[1]
    left = sT[pl.ds(pl.multiple_of(h * half, half), half), : x.shape[0]]
    for j in range(0, hid, 256):
        block = dot(left, x[:, j : j + 256])
        for p in range(2):
            slot = pl.ds((flip + p - 2 * flip * p) * 16, 16)
            for c in range(2):
                n = j // LANES + c
                out[slot, n * 16 : (n + 1) * 16, :] = block[
                    p * 256 : (p + 1) * 256, c * LANES : (c + 1) * LANES
                ].reshape(16, 16, LANES)
    for i in range(4):
        p = i // 2
        slot = (flip + p - 2 * flip * p) * 16 + (i % 2) * 8
        rows8 = e[pl.ds(pl.multiple_of(h * 32 + i * 8, 8), 8), :]
        for n in range(8):
            out[slot + n, 128:136, :] = rows8[:, n * LANES : (n + 1) * LANES]


def mine_kernel(place, sT, x, e, out):
    tile_half(place, place[0], sT, x, e, out)


def plane_sum_kernel(arrived, out):
    total = arrived[0]
    for i in range(1, arrived.shape[0]):
        total = total + arrived[i]
    out[...] = total


def line_sum_kernel(own, near, far, both, out):
    total = (own[...] + near[...]) + (far[...] + both[...])
    for i in range(out.shape[0]):
        out[i] = total


def lay_out(place, part, h, gh_far, e, sem):
    units = part.shape[0]
    flip = place[1]
    copies = []
    for p in range(2):
        slot = pl.ds((flip + p - 2 * flip * p) * 16, 16)
        at = pl.ds(h * units + p * 16, 16)
        for n in range(8):
            copies.append(
                started(
                    part.at[slot, n * 16 : (n + 1) * 16, :],
                    gh_far.at[at, :, n * LANES : (n + 1) * LANES],
                    sem.at[p * 8 + n],
                )
            )
    for i in range(4):
        p = i // 2
        slot = (flip + p - 2 * flip * p) * 16 + (i % 2) * 8
        at8 = pl.ds(pl.multiple_of(h * 32 + i * 8, 8), 8)
        for n in range(8):
            e[at8, n * LANES : (n + 1) * LANES] = part[slot + n, 128:136, :]
    return copies


def first_half_kernel(place, mine, gh_far, e, sem):
    e[...] = jnp.zeros_like(e)
    for copy in lay_out(place, mine, place[0], gh_far, e, sem):
        copy.wait()


def second_half_kernel(place, other, e_in, gh_in, gh_far, ga_far, gd_far, e, ga, gd, sem):
    e[...] = e_in[...]
    copies = lay_out(place, other, 1 - place[0], gh_far, e, sem)
    ga[...] = e[A_ROW : A_ROW + ga.shape[0], :]
    copies.append(started(ga, ga_far, sem.at[16]))
    gd[...] = e[0 : gd.shape[0], :]
    copies.append(started(gd, gd_far, sem.at[17]))
    for copy in copies:
        copy.wait()


def shifted(array, axis, by):
    size = lax.axis_size(axis)
    return lax.ppermute(array, axis, [(i, (i + by) % size) for i in range(size)])


def of_group(part):
    return [part] + [shifted(part, "y", by) for by in (2, 1, 3)]


def swapped(tiles, axis):
    return lax.all_to_all(tiles, axis, split_axis=0, concat_axis=0, tiled=True)


def along_z(array, to):
    return lax.ppermute(array, LINE, [(z, to(z)) for z in range(8)])


def beside(z):
    return (z + 1 if z % 2 else z - 1) % 8


def across(z):
    return (z + 4) % 8


def body(embed, actions, rewards, ends, behaviour, w_hidden, w_action, w_heads):
    rows, hid = embed.shape
    steps = actions.shape[1]
    count = w_action.shape[0]
    groups = lax.axis_size("y")
    devices = lax.axis_size(ALL)
    place = jnp.stack([lax.axis_index("core"), lax.axis_index("zh") % 2]).astype(jnp.int32)

    s, t, out, ssq, act, whp = kernel_call(
        unroll_kernel,
        [
            ((steps * rows, hid), BF16),
            (((steps - 1) * rows, hid), F32),
            ((48, (steps + 1) * rows), F32),
            ((8, LANES), F32),
            ((steps, rows), jnp.int32),
            ((48, hid), BF16),
        ],
        (embed, actions.T, w_hidden, w_action, w_heads.T),
        (
            pltpu.VMEM((rows, hid), BF16),
            pltpu.VMEM((hid, hid), BF16),
            pltpu.VMEM((count, hid), BF16),
            pltpu.VMEM((2 * count, hid), BF16),
            pltpu.VMEM(((steps - 1) * rows, hid), F32),
            pltpu.VMEM((32, hid), BF16),
            pltpu.VMEM((48, hid), F32),
            pltpu.VMEM((40, hid), F32),
            pltpu.SemaphoreType.DMA((5,)),
            pltpu.SemaphoreType.DMA((steps - 1,)),
        ),
        far=range(5),
        far_outs=(1,),
    )
    ssqs = of_group(ssq)
    per_action = ((count, steps * rows), F32)
    targets, pis, advs, dqs, sT = kernel_call(
        targets_kernel,
        [((steps, rows), F32), per_action, per_action, per_action, ((hid, steps * rows), BF16)],
        (rewards.T, ends.T, jnp.transpose(behaviour, (1, 2, 0)), act, s, out),
        (
            pltpu.VMEM((steps, rows), F32),
            pltpu.VMEM((steps, rows), jnp.int32),
            pltpu.VMEM((steps, count, rows), F32),
            pltpu.VMEM((steps, rows), F32),
            pltpu.SemaphoreType.DMA((4,)),
        ),
        far=range(3),
        far_outs=(0,),
    )

    def weights_body(*refs):
        weights_kernel(groups, devices, *refs)

    a, b, mass = kernel_call(
        weights_body,
        [((48, steps * rows), F32), ((Q_ROW, steps * rows), F32), ((8, LANES), F32)],
        (act, pis, advs, dqs, *ssqs),
    )
    masses = of_group(mass)

    t, wh, oh = kernel_call(
        fetch_kernel,
        [(t.shape, F32), (w_hidden.shape, BF16), ((32, (steps - 1) * rows), BF16)],
        (t, w_hidden, act, mass),
        (pltpu.SemaphoreType.DMA((2,)),),
        far=(0, 1),
    )

    def gradient_body(*refs):
        gradient_kernel(groups, count, *refs)

    parts = ((32, 136, LANES), F32)
    other, x, extra = kernel_call(
        gradient_body,
        [parts, (((steps - 1) * rows, hid), BF16), ((64, hid), F32)],
        (place, act, a, b, *masses, s, sT, t, wh, whp, oh),
        (
            pltpu.VMEM((48, steps * rows), F32),
            pltpu.VMEM((48, steps * rows), BF16),
        ),
        scalars=1,
    )
    arriving = shifted(other, "core", 1)
    (mine,) = kernel_call(mine_kernel, [parts], (place, sT, x, extra), scalars=1)
    chip = mine + arriving
    (own,) = kernel_call(plane_sum_kernel, [((136, LANES), F32)], (swapped(chip, NEAR),))
    far = along_z(own, across)
    both = along_z(own, lambda z: across(beside(z)))
    near = along_z(own, beside)
    (whole,) = kernel_call(line_sum_kernel, [parts], (own, near, far, both))
    mine = swapped(whole, NEAR)
    other = shifted(mine, "core", 1)
    copied = pltpu.SemaphoreType.DMA((16,))
    tiles = ((64, 16, hid), F32)
    partly, extra = kernel_call(
        first_half_kernel,
        [tiles, ((64, hid), F32)],
        (place, mine),
        (copied,),
        scalars=1,
        far_outs=(0,),
    )
    grad_hidden, grad_action, grad_heads = kernel_call(
        second_half_kernel,
        [tiles, (w_action.shape, F32), (w_heads.shape[::-1], F32)],
        (place, other, extra, partly),
        (
            pltpu.VMEM((64, hid), F32),
            pltpu.VMEM(w_action.shape, F32),
            pltpu.VMEM(w_heads.shape[::-1], F32),
            pltpu.SemaphoreType.DMA((18,)),
        ),
        scalars=1,
        far=(3,),
        far_outs=(0, 1, 2),
        aliases={3: 0},
    )
    return (grad_hidden.reshape(hid, hid), grad_action, grad_heads.T, targets.T)


def solution(mesh):
    torus = Mesh(mesh.devices.reshape(4, 2, 4, 2, mesh.shape["batch"]), ALL)
    return jax.shard_map(
        body,
        mesh=torus,
        in_specs=(
            P(ALL, None),
            P(ALL, None),
            P(ALL, None),
            P(ALL, None),
            P(ALL, None, None),
            P(),
            P(),
            P(),
        ),
        out_specs=(P(), P(), P(), P(ALL, None)),
        check_vma=False,
    )
```
